128 devices in a mesh: dp: 4 (over x), fsdp: 8 (over y, core), enc: 4 (over z).
Axes of the slice: x: 4, y: 4, z: 4, core: 2. Of those that a mesh axis runs over, the one named last changes fastest.
Arguments:
- hidden: bfloat16 [32768, 8192], P(('dp', 'fsdp', 'enc')), may hold values from -40 to 40
- residual_gradient: bfloat16 [32768, 8192], P(('dp', 'fsdp', 'enc')), may hold values from -3 to 3
- value_output_gradient: bfloat16 [32768, 1024], P(('dp', 'fsdp', 'enc')), may hold values from -6 to 6
- attention_norm_gain: float32 [8192], replicated, may hold values from 0.1 to 1.9
- value_frozen_weight: bfloat16 [8192, 1024], P('fsdp'), may hold values from -0.0625 to 0.0625
- value_down_factor: bfloat16 [8192, 16], replicated, may hold values from -0.0625 to 0.0625
- value_up_factor: bfloat16 [16, 1024], replicated, may hold values from -0.29882812 to 0.29882812
- merger_frozen_weight: bfloat16 [5120, 8192], P(None, ('fsdp', 'enc')), may hold values from -0.078125 to 0.078125
- merger_down_factor: bfloat16 [5120, 16], replicated, may hold values from -0.078125 to 0.078125
- merger_up_factor: bfloat16 [16, 8192], P(None, ('fsdp', 'enc')), may hold values from -0.29882812 to 0.29882812
- merger_saved_preactivation: bfloat16 [4096, 5120], P(('dp', 'fsdp', 'enc')), may hold values from -5 to 5
- image_token_counts: int32 [128], P('dp'), may hold values from 8 to 16, as said below
- image_encoder_owner: int32 [128], P('dp'), may hold values from 0 to 31, as said below
- image_first_rows: int32 [128], P(('dp', 'fsdp', 'enc')), may hold values from 0 to 255, as said below
Outputs:
- layer_input_gradient: bfloat16 [32768, 8192], P(('dp', 'fsdp', 'enc'))
- preactivation_gradient: bfloat16 [4096, 5120], P(('dp', 'fsdp', 'enc'))
- value_down_gradient: float32 [8192, 16], replicated
- value_up_gradient: float32 [16, 1024], replicated
- merger_down_gradient: float32 [5120, 16], replicated
- merger_up_gradient: float32 [16, 8192], P(None, ('fsdp', 'enc'))
The draws below stay inside these ranges and needn't reach their ends.
Inputs may be any that keep to these rules, and one draw needn't show every extreme that they name: `image_token_counts`: within each data replica some encoder device owns exactly 2 images, all of 16 visual tokens, so its rows fill all 32; no other device owns more than 2 images. `image_encoder_owner`: encoder devices are numbered within the data replica in mesh order. `image_first_rows`: images of one device lie inside its 256 rows in increasing order and don't intersect.
All inputs are finite; a program needn't handle non-finite values.
Results may differ from the reference program's by a relative error of at most 0.0085.
Values may be sent and summed in bfloat16 or wider, within the bound.
A program may use at most 192 MiB of HBM per device.

```python
import jax
import jax.numpy as jnp
from jax import lax

MODEL_WIDTH = 8192
VALUE_WIDTH = 1024
MERGE = 5120
ADAPTER_RANK = 16
TOK_DEV = 256
IMG_DEV = 1
MAXIMG = 16
OWNERS = 32
OCAP = 32
TOKENS = 32768
OWN_ROWS = 4096
N_DP = 4
N_FSDP = 8
N_ENC = 4


def image_layout(key):
    group_keys = jax.random.split(jax.random.fold_in(key, 11), N_DP)

    def one_group(group_key):
        subkeys = jax.random.split(group_key, 5)
        per_group = OWNERS * IMG_DEV
        busiest_load = 2 * IMG_DEV
        busiest = jax.random.randint(subkeys[0], (), 0, OWNERS)
        others = (busiest + 1 + jnp.arange((OWNERS - 1) * busiest_load) // busiest_load) % OWNERS
        others = jax.random.permutation(subkeys[1], others)[:per_group - busiest_load]
        listed = jnp.concatenate([jnp.zeros((busiest_load,), jnp.int32) + busiest, others.astype(jnp.int32)])
        listed = jax.random.permutation(subkeys[2], listed).astype(jnp.int32)
        counts = jax.random.randint(subkeys[3], (per_group,), MAXIMG // 2, MAXIMG + 1)
        counts = jnp.where(listed == busiest, MAXIMG, counts).astype(jnp.int32)
        spare_rows = (TOK_DEV - IMG_DEV * MAXIMG) // IMG_DEV
        text_gaps = jax.random.randint(subkeys[4], (OWNERS, IMG_DEV), 0, spare_rows + 1)
        shaped = counts.reshape(OWNERS, IMG_DEV)
        offsets = jnp.cumsum(text_gaps + shaped, axis=1) - shaped
        return (counts, listed, offsets.reshape(-1).astype(jnp.int32))
    counts, listed, offsets = jax.vmap(one_group)(group_keys)
    return (counts.reshape(-1).astype(jnp.int32), listed.reshape(-1).astype(jnp.int32), offsets.reshape(-1).astype(jnp.int32))


def draw_image_token_counts(key, part):
    return image_layout(key)[0]


def draw_image_encoder_owner(key, part):
    return image_layout(key)[1]


def draw_image_first_rows(key, part):
    return image_layout(key)[2]


def draw_hidden(key, part):
    subkeys = jax.random.split(jax.random.fold_in(key, 3), 3)
    values = jax.random.normal(subkeys[0], (TOKENS, MODEL_WIDTH), jnp.float32)
    row_scale = jnp.exp(jax.random.uniform(subkeys[1], (TOKENS, 1), jnp.float32, -1.2, 1.2))
    column_scale = jnp.exp(jax.random.uniform(subkeys[2], (1, MODEL_WIDTH), jnp.float32, -1.2, 1.2))
    return jnp.clip(values * row_scale * column_scale, -40.0, 40.0).astype(jnp.bfloat16)


def levels(rng, extent, shards, low, largest):
    level = 1.0
    for axis_at, parts in shards:
        steps = jax.random.uniform(jax.random.fold_in(jax.random.fold_in(rng, 6), axis_at), (parts,), jnp.float32, low / len(shards), largest / len(shards))
        level = level * jnp.repeat(jnp.exp(steps), extent[axis_at] // parts).reshape((-1,) + (1,) * (len(extent) - 1 - axis_at))
    return level


def gaussian(rng, shape, width, reach, shards=(), held_as=jnp.bfloat16):
    level = levels(rng, shape, shards, -0.22, 0.18) if shards else 1.0
    values = jax.random.normal(rng, shape, jnp.float32) * width * level
    return jnp.minimum(jnp.maximum(values, -reach), reach).astype(held_as)


def setup_inputs(seed: int = 0) -> dict:
    key_of = jax.random.split(jax.random.key(seed), 15)
    hidden = draw_hidden(jax.random.fold_in(key_of[14], 71), 0)
    residual_gradient = gaussian(key_of[1], (TOKENS, MODEL_WIDTH), 0.5, 3.0, ((0, 128),))
    value_output_gradient = gaussian(key_of[2], (TOKENS, VALUE_WIDTH), 1.0, 6.0, ((0, 128),))
    attention_norm_gain = jnp.clip(1.0 + 0.18 * jax.random.normal(key_of[3], (MODEL_WIDTH,), jnp.float32), 0.1, 1.9)
    value_frozen_weight = gaussian(key_of[4], (MODEL_WIDTH, VALUE_WIDTH), MODEL_WIDTH ** -0.5, 0.0625, ((0, 8),))
    value_down_factor = gaussian(key_of[5], (MODEL_WIDTH, ADAPTER_RANK), MODEL_WIDTH ** -0.5, 0.0625)
    value_up_factor = gaussian(key_of[6], (ADAPTER_RANK, VALUE_WIDTH), 0.05, 0.29882812)
    merger_frozen_weight = gaussian(key_of[7], (MERGE, MODEL_WIDTH), MERGE ** -0.5, 0.078125, ((1, 32),))
    merger_down_factor = gaussian(key_of[8], (MERGE, ADAPTER_RANK), MERGE ** -0.5, 0.078125)
    merger_up_factor = gaussian(key_of[9], (ADAPTER_RANK, MODEL_WIDTH), 0.05, 0.29882812, ((1, 32),))
    merger_saved_preactivation = gaussian(key_of[10], (OWN_ROWS, MERGE), 1.0, 5.0, ((0, 128),))
    image_token_counts = draw_image_token_counts(jax.random.fold_in(key_of[14], 71), 0)
    image_encoder_owner = draw_image_encoder_owner(jax.random.fold_in(key_of[14], 71), 0)
    image_first_rows = draw_image_first_rows(jax.random.fold_in(key_of[14], 71), 0)
    return dict(hidden=hidden, residual_gradient=residual_gradient, value_output_gradient=value_output_gradient, attention_norm_gain=attention_norm_gain, value_frozen_weight=value_frozen_weight, value_down_factor=value_down_factor, value_up_factor=value_up_factor, merger_frozen_weight=merger_frozen_weight, merger_down_factor=merger_down_factor, merger_up_factor=merger_up_factor, merger_saved_preactivation=merger_saved_preactivation, image_token_counts=image_token_counts, image_encoder_owner=image_encoder_owner, image_first_rows=image_first_rows)


adapter_scale = 2.0
norm_eps = 1e-06

def gelu_parts(preact):
    normal_cdf = 0.5 * (1.0 + lax.erf(preact * 0.7071067811865476))
    normal_pdf = jnp.exp(-0.5 * preact * preact) * 0.3989422804014327
    return (normal_cdf, normal_pdf)

def owner_layout(image_token_counts, image_encoder_owner, owner_count, owner_room, slot_len):
    total_images = image_token_counts.shape[0]
    image_ids = jnp.arange(total_images).astype(jnp.int32)
    same_owner = image_encoder_owner[:, None] == image_encoder_owner[None, :]
    earlier = image_ids[None, :] < image_ids[:, None]
    starts = lax.optimization_barrier(jnp.sum(jnp.where(same_owner & earlier, image_token_counts[None, :], 0), axis=1)).astype(jnp.int32)
    row_index = jnp.arange(owner_count * owner_room).astype(jnp.int32)
    row_owner = (row_index // owner_room).astype(jnp.int32)
    row_place = (row_index % owner_room).astype(jnp.int32)
    matches = (row_owner[:, None] == image_encoder_owner[None, :]) & (row_place[:, None] >= starts[None, :]) & (row_place[:, None] < (starts + image_token_counts)[None, :])
    source = lax.optimization_barrier(jnp.sum(jnp.where(matches, image_ids[None, :] * slot_len + row_place[:, None] - starts[None, :], 0), axis=1)).astype(jnp.int32)
    valid_rows = jnp.any(matches, axis=1)
    return (source, valid_rows)

def take_slots(layer_input_gradient, counts_in, offsets_in):
    padded = jnp.concatenate([layer_input_gradient, jnp.zeros((MAXIMG, layer_input_gradient.shape[1]), layer_input_gradient.dtype)], axis=0)
    pieces = []
    for image_index in range(offsets_in.shape[0]):
        window = lax.dynamic_slice_in_dim(padded, offsets_in[image_index], MAXIMG, 0)
        inside = jnp.arange(MAXIMG) < counts_in[image_index]
        pieces.append(jnp.where(inside[:, None], window, jnp.zeros_like(window)))
    return jnp.concatenate(pieces, axis=0)

def decoder_layer_block(incoming_rows, residual_input, value_incoming, attention_norm_gain, passed_gradient, value_down_factor, value_up_factor):
    values = incoming_rows.astype(jnp.float32)
    inverse = lax.rsqrt(lax.optimization_barrier(jnp.mean(values * values, axis=1, keepdims=True)) + norm_eps)
    gain_values = attention_norm_gain.astype(jnp.float32)
    normalized_input = (values * inverse * gain_values).astype(jnp.bfloat16)
    value_low_product = jnp.dot(value_incoming, value_up_factor.T, preferred_element_type=jnp.float32).astype(jnp.bfloat16)
    normalized_gradient = passed_gradient.astype(jnp.float32) + adapter_scale * jnp.dot(value_low_product, value_down_factor.T, preferred_element_type=jnp.float32)
    gained = gain_values * normalized_gradient
    layer_input_gradient = (residual_input.astype(jnp.float32) + inverse * gained - values * inverse ** 3 * lax.optimization_barrier(jnp.mean(values * gained, axis=1, keepdims=True))).astype(jnp.bfloat16)
    projected_rows = jnp.dot(normalized_input, value_down_factor, preferred_element_type=jnp.float32).astype(jnp.bfloat16)
    up_term = lax.dot_general(projected_rows, value_incoming, (((0,), (0,)), ((), ())), preferred_element_type=jnp.float32)
    down_term = lax.dot_general(normalized_input, value_low_product, (((0,), (0,)), ((), ())), preferred_element_type=jnp.float32)
    return (layer_input_gradient, down_term, up_term)

def reference(hidden, residual_gradient, value_output_gradient, attention_norm_gain, value_frozen_weight, value_down_factor, value_up_factor, merger_frozen_weight, merger_down_factor, merger_up_factor, merger_saved_preactivation, image_token_counts, image_encoder_owner, image_first_rows):
    device_total = N_DP * N_FSDP * N_ENC
    owner_count = N_FSDP * N_ENC
    gradient_scale = 256.0 / TOKENS
    value_transposed = value_frozen_weight.T

    def device_step(running, inputs):
        incoming_rows, residual_input, value_incoming, counts_in, offsets_in = inputs
        passed_gradient = jnp.dot(value_incoming, value_transposed, preferred_element_type=jnp.float32).astype(jnp.bfloat16)
        layer_input_gradient, down_term, up_term = decoder_layer_block(incoming_rows, residual_input, value_incoming, attention_norm_gain, passed_gradient, value_down_factor, value_up_factor)
        slots_out = take_slots(layer_input_gradient, counts_in, offsets_in)
        return ((running[0] + down_term, running[1] + up_term), (layer_input_gradient, slots_out))
    start_sums = (jnp.zeros((MODEL_WIDTH, ADAPTER_RANK), jnp.float32), jnp.zeros((ADAPTER_RANK, VALUE_WIDTH), jnp.float32))
    scanned = (hidden.reshape(device_total, TOK_DEV, MODEL_WIDTH), residual_gradient.reshape(device_total, TOK_DEV, MODEL_WIDTH), value_output_gradient.reshape(device_total, TOK_DEV, VALUE_WIDTH), image_token_counts.reshape(device_total, IMG_DEV), image_first_rows.reshape(device_total, IMG_DEV))
    sums, outputs = lax.scan(device_step, start_sums, scanned)
    layer_input_gradient = outputs[0].reshape(TOKENS, MODEL_WIDTH)
    group_slots = outputs[1].reshape(N_DP, owner_count * IMG_DEV * MAXIMG, MODEL_WIDTH)
    merger_weight_transposed = merger_frozen_weight.T
    merger_b_transposed = merger_up_factor.T
    merger_down_widened = merger_down_factor.astype(jnp.float32).T

    def group_step(inputs):
        slots_in, counts_in, owners_in, preact_in = inputs
        source, valid_rows = owner_layout(counts_in, owners_in, owner_count, OCAP, MAXIMG)
        visual_tokens = jnp.where(valid_rows[:, None], jnp.take(slots_in, source, axis=0), jnp.zeros((), slots_in.dtype))
        merger_low_product = jnp.dot(visual_tokens, merger_b_transposed, preferred_element_type=jnp.float32)
        combined_gradient = jnp.dot(visual_tokens, merger_weight_transposed, preferred_element_type=jnp.float32) + adapter_scale * jnp.dot(merger_low_product, merger_down_widened, precision=lax.Precision.HIGHEST)
        preact = preact_in.astype(jnp.float32)
        normal_cdf, normal_pdf = gelu_parts(preact)
        preactivation_gradient = (combined_gradient * (normal_cdf + preact * normal_pdf)).astype(jnp.bfloat16)
        activation = (preact * normal_cdf).astype(jnp.bfloat16)
        act_low = jnp.dot(activation, merger_down_factor, preferred_element_type=jnp.float32).astype(jnp.bfloat16)
        term_b2 = lax.dot_general(act_low, visual_tokens, (((0,), (0,)), ((), ())), preferred_element_type=jnp.float32)
        term_a2 = lax.dot_general(activation, merger_low_product.astype(jnp.bfloat16), (((0,), (0,)), ((), ())), preferred_element_type=jnp.float32)
        return (preactivation_gradient, term_b2, term_a2)
    grouped = (group_slots, image_token_counts.reshape(N_DP, -1), image_encoder_owner.reshape(N_DP, -1), merger_saved_preactivation.reshape(N_DP, owner_count * OCAP, MERGE))
    pre_grads, terms_b2, terms_a2 = lax.map(group_step, grouped)
    scale_factor = gradient_scale * adapter_scale
    return (layer_input_gradient, pre_grads.reshape(OWN_ROWS, MERGE), scale_factor * sums[0], scale_factor * sums[1], scale_factor * lax.optimization_barrier(jnp.sum(terms_a2, axis=0)), scale_factor * lax.optimization_barrier(jnp.sum(terms_b2, axis=0)))
```

```python
import functools

import jax
import jax.numpy as jnp
from jax import lax
from jax.experimental import pallas as pl
from jax.experimental.pallas import tpu as pltpu
from jax.sharding import PartitionSpec as P

MAXIMG = 16
adapter_scale = 2.0
norm_eps = 1e-06
F32, BF16 = jnp.float32, jnp.bfloat16
MESH = pl.DeviceIdType.MESH
VMEM = pl.BlockSpec(memory_space=pltpu.VMEM)
ANY = pl.BlockSpec(memory_space=pl.ANY)


def dot_nt(a, b):
    return lax.dot_general(a, b, (((1,), (1,)), ((), ())), preferred_element_type=F32)


def dot_tn(a, b):
    return lax.dot_general(a, b, (((0,), (0,)), ((), ())), preferred_element_type=F32)


def wrap(v, n):
    return lax.rem(v + n, n)


def place():
    f = lax.axis_index("fsdp")
    return lax.axis_index("dp"), f // 2, lax.axis_index("enc"), lax.rem(f, 2)


class Links:
    def __init__(self, send_sems, recv_sems):
        self.x, self.y, self.z, self.c = place()
        self.send_sems, self.recv_sems = send_sems, recv_sems
        self.made = []

    def peer(self, axis, step):
        if axis == "x":
            return {"dp": wrap(self.x + step, 4)}
        if axis == "z":
            return {"enc": wrap(self.z + step, 4)}
        if axis == "y":
            return {"fsdp": 2 * wrap(self.y + step, 4) + self.c}
        return {"fsdp": 2 * self.y + 1 - self.c}

    def send(self, axis, step, src, dst):
        k = len(self.made)
        copy = pltpu.make_async_remote_copy(
            src_ref=src,
            dst_ref=dst,
            send_sem=self.send_sems.at[k],
            recv_sem=self.recv_sems.at[k],
            device_id=self.peer(axis, step),
            device_id_type=MESH,
        )
        copy.start()
        self.made.append(copy)
        return copy

    def finish(self):
        for copy in self.made:
            copy.wait_send()

    def meet(self, peers):
        barrier = pltpu.get_barrier_semaphore()
        for axis, step in peers:
            pl.semaphore_signal(barrier, inc=1, device_id=self.peer(axis, step), device_id_type=MESH)
        pl.semaphore_wait(barrier, len(peers))


def image_kernel(
    vimg, ximg, rimg, keep, gain, wsh, up, down_t, act_low, wm, mup,
    vrecv, alow, wm_other, mup_other,
    vall, tout, timg, gained, visout,
    s1, r1, s2, r2, s3, r3, s4, r4, s5, r5, keep_sem,
):
    x, y, z, c = place()
    f = 2 * y + c
    me = f * 4 + z
    barrier = pltpu.get_barrier_semaphore()

    def greet(j, carry):
        d = lax.rem(me + j, 32)
        pl.semaphore_signal(
            barrier, inc=1, device_id={"fsdp": d // 4, "enc": lax.rem(d, 4)}, device_id_type=MESH
        )
        return carry

    lax.fori_loop(1, 32, greet, 0)
    pl.semaphore_wait(barrier, 31)

    def row(j, slot):
        return pltpu.make_async_remote_copy(
            src_ref=vimg, dst_ref=vall.at[slot], send_sem=s1.at[j], recv_sem=r1.at[j],
            device_id={"fsdp": lax.rem(f + j, 8)}, device_id_type=MESH,
        )

    def back(j, slot):
        return pltpu.make_async_remote_copy(
            src_ref=tout.at[lax.rem(f + j, 8)], dst_ref=timg.at[slot], send_sem=s2.at[j],
            recv_sem=r2.at[j], device_id={"fsdp": lax.rem(f + j, 8)}, device_id_type=MESH,
        )

    def spread(j, slot):
        d = lax.rem(me + j, 32)
        return pltpu.make_async_remote_copy(
            src_ref=visout.at[d // 8, lax.rem(d, 4)], dst_ref=vrecv.at[slot], send_sem=s3.at[j],
            recv_sem=r3.at[j], device_id={"fsdp": d // 4, "enc": lax.rem(d, 4)}, device_id_type=MESH,
        )

    def low_out(j, slot):
        d = lax.rem(me + j, 32)
        return pltpu.make_async_remote_copy(
            src_ref=act_low, dst_ref=alow.at[slot], send_sem=s4.at[j], recv_sem=r4.at[j],
            device_id={"fsdp": d // 4, "enc": lax.rem(d, 4)}, device_id_type=MESH,
        )

    def over(lo, hi, act):
        def step(j, carry):
            act(j)
            return carry

        lax.fori_loop(lo, hi, step, 0)

    over(1, 8, lambda j: row(j, f).start())
    wide = pltpu.make_async_remote_copy(
        src_ref=wm, dst_ref=wm_other, send_sem=s5.at[0], recv_sem=r5.at[0],
        device_id={"fsdp": 2 * y + 1 - c}, device_id_type=MESH,
    )
    thin = pltpu.make_async_remote_copy(
        src_ref=mup, dst_ref=mup_other, send_sem=s5.at[1], recv_sem=r5.at[1],
        device_id={"fsdp": 2 * y + 1 - c}, device_id_type=MESH,
    )
    wide.start()
    thin.start()
    over(1, 32, lambda j: low_out(j, me).start())
    alow[me] = act_low[...]
    vall[f] = vimg[...]
    low = dot_nt(vimg[...], up[...]).astype(BF16)
    over(1, 8, lambda j: row(j, lax.rem(f - j + 8, 8)).wait_recv())
    through = dot_nt(vall[...].reshape(128, 1024), wsh[...]).astype(BF16).reshape(8, 16, 1024)
    tout[...] = through
    over(1, 8, lambda j: back(j, f).start())
    timg[f] = tout[f]
    squares = jnp.zeros((16, 1), F32)
    for k in range(8):
        xs = ximg[:, k * 1024 : (k + 1) * 1024].astype(F32)
        squares = squares + jnp.sum(xs * xs, axis=1, keepdims=True)
    inverse = lax.rsqrt(squares * (1.0 / 8192) + norm_eps)
    over(1, 8, lambda j: back(j, lax.rem(f - j + 8, 8)).wait_recv())
    total = jnp.zeros((16, 1), F32)
    for k in range(8):
        cols = slice(k * 1024, (k + 1) * 1024)
        grad = timg[k].astype(F32) + adapter_scale * jnp.dot(
            low, down_t[k], preferred_element_type=F32
        )
        g = gain[k] * grad
        gained[k] = g
        total = total + jnp.sum(ximg[:, cols].astype(F32) * g, axis=1, keepdims=True)
    drop = inverse * inverse * inverse * (total * (1.0 / 8192))
    inside = keep[:, 0:1] > 0.5
    for k in range(8):
        cols = slice(k * 1024, (k + 1) * 1024)
        rows = rimg[:, cols].astype(F32) + inverse * gained[k] - ximg[:, cols].astype(F32) * drop
        rows = jnp.where(inside, rows, 0.0).astype(BF16)
        for b in range(4):
            visout[k // 2, b, k % 2] = rows[:, b * 256 : (b + 1) * 256]
    over(1, 32, lambda j: spread(j, me).start())
    vrecv[me] = visout[y, z]
    over(1, 32, lambda j: spread(j, lax.rem(me - j + 32, 32)).wait_recv())
    over(1, 32, lambda j: low_out(j, lax.rem(me - j + 32, 32)).wait_recv())
    wide.wait_recv()
    thin.wait_recv()
    over(1, 8, lambda j: row(j, f).wait_send())
    over(1, 8, lambda j: back(j, f).wait_send())
    over(1, 32, lambda j: spread(j, me).wait_send())
    over(1, 32, lambda j: low_out(j, me).wait_send())
    wide.wait_send()
    thin.wait_send()


def image_chain(vimg, ximg, rimg, keep, gain, wsh, up, down_t, act_low, wm, mup):
    dma = pltpu.SemaphoreType.DMA
    return pl.pallas_call(
        image_kernel,
        out_shape=(
            jax.ShapeDtypeStruct((32, 2, 16, 256), BF16),
            jax.ShapeDtypeStruct((32, 32, 128), BF16),
            jax.ShapeDtypeStruct(wm.shape, BF16),
            jax.ShapeDtypeStruct(mup.shape, BF16),
        ),
        in_specs=[VMEM] * 9 + [ANY, ANY],
        out_specs=(VMEM, VMEM, ANY, ANY),
        scratch_shapes=[
            pltpu.VMEM((8, 16, 1024), BF16),
            pltpu.VMEM((8, 16, 1024), BF16),
            pltpu.VMEM((8, 16, 1024), BF16),
            pltpu.VMEM((8, 16, 1024), F32),
            pltpu.VMEM((4, 4, 2, 16, 256), BF16),
            dma((8,)), dma((8,)), dma((8,)), dma((8,)),
            dma((32,)), dma((32,)), dma((32,)), dma((32,)),
            dma((2,)), dma((2,)), dma((1,)),
        ],
        compiler_params=pltpu.CompilerParams(collective_id=0, has_side_effects=True),
        name="image_chain",
    )(vimg, ximg, rimg, keep, gain, wsh, up, down_t, act_low, wm, mup)


def main_kernel(
    scale_factor,
    hidden, resid, wsh, v, up, gain, down_t,
    out, down_term, up_term,
    wbuf, xb, rb, gained, send_sems, recv_sems, local_sems, out_sems,
):
    links = Links(send_sems, recv_sems)
    x, y, z, c = links.x, links.y, links.z, links.c
    own = pltpu.make_async_copy(wsh, wbuf.at[c, 0], local_sems.at[0])
    own.start()
    loads = []
    for k in range(8):
        cols = pl.ds(k * 1024, 1024)
        a = pltpu.make_async_copy(hidden.at[:, cols], xb.at[k], local_sems.at[1 + k])
        b = pltpu.make_async_copy(resid.at[:, cols], rb.at[k], local_sems.at[9 + k])
        a.start()
        b.start()
        loads.append((a, b))
    links.meet([("x", 1), ("x", -1), ("y", 1), ("y", -1), ("z", 1), ("z", -1), ("c", 0)])
    own.wait()

    def rows(half, a, b, extra, count):
        at = ((half * 4 + a) * 4 + b) * 32 + extra
        return pl.ds(pl.multiple_of(at, 16), count)

    def at(j, span):
        return wbuf.at[c, j, span]

    inner = ((0, z, x), (1, x, z))
    first = ("x", "z")
    second = ("z", "x")

    def piece(half, step, extra, count):
        _, a, b = inner[half]
        return rows(half, a, wrap(b + step, 4), extra, count)

    def block(half, step, extra, count):
        _, a, _ = inner[half]
        return rows(half, wrap(a + step, 4), 0, extra, count)

    y1 = []
    for h in range(2):
        span = piece(h, 0, 0, 32)
        y1.append(
            (links.send("y", 1, at(0, span), at(3, span)), links.send("y", -1, at(0, span), at(1, span)))
        )
    across = {0: links.send("c", 0, wbuf.at[c, 0], wbuf.at[c, 0])}

    squares = jnp.zeros((256, 1), F32)
    for k in range(8):
        loads[k][0].wait()
        xs = xb[k].astype(F32)
        squares = squares + jnp.sum(xs * xs, axis=1, keepdims=True)
    inverse = lax.rsqrt(squares * (1.0 / 8192) + norm_eps)

    a1, a2, b1, b2 = {}, {}, {}, {}

    def start_a1(j):
        a1[j] = []
        for h in range(2):
            span = piece(h, 0, 0, 32)
            for step in (1, -1):
                a1[j].append(links.send(first[h], step, at(j, span), at(j, span)))

    def start_a2(j):
        a2[j] = []
        for h in range(2):
            for step, extra in ((1, 0), (-1, 16)):
                span = piece(h, -step, extra, 16)
                a2[j].append(links.send(first[h], step, at(j, span), at(j, span)))

    def start_b1(j):
        b1[j] = []
        for h in range(2):
            span = block(h, 0, 0, 128)
            for step in (1, -1):
                b1[j].append(links.send(second[h], step, at(j, span), at(j, span)))

    def start_b2(j):
        b2[j] = []
        for h in range(2):
            for step, extra in ((1, 0), (-1, 64)):
                span = block(h, -step, extra, 64)
                b2[j].append(links.send(second[h], step, at(j, span), at(j, span)))

    def arrived(copies):
        for copy in copies:
            copy.wait_recv()

    for pair in y1:
        arrived(pair)
    y2 = []
    for h in range(2):
        for step, j, extra in ((1, 3, 0), (-1, 1, 16)):
            span = piece(h, 0, extra, 16)
            y2.append(links.send("y", step, at(j, span), at(2, span)))
    start_a1(3)
    start_a1(1)

    low = dot_nt(v[...], up[...]).astype(BF16)
    low_t = dot_nt(up[...], v[...]).astype(BF16)
    arrived(y2)
    start_a1(2)

    projected_t = jnp.zeros((16, 256), F32)

    def normed_block(k, projected_t):
        normed = (xb[k].astype(F32) * inverse * gain[k]).astype(BF16)
        down_term[k] = scale_factor * jnp.dot(low_t, normed, preferred_element_type=F32)
        return projected_t + dot_nt(down_t[k], normed)

    def through_block(cs, j, total):
        k = 2 * lax.rem(y + j, 4) + cs
        through = dot_nt(v[...], wbuf[cs, j]).astype(BF16)
        grad = through.astype(F32) + adapter_scale * jnp.dot(
            low, down_t[k], preferred_element_type=F32
        )
        g = gain[k] * grad
        gained[k] = g
        return total + jnp.sum(xb[k].astype(F32) * g, axis=1, keepdims=True)

    total = jnp.zeros((256, 1), F32)
    order = (3, 1, 2)
    for n, j in enumerate(order):
        arrived(a1[j])
        start_a2(j)
        projected_t = normed_block(n, projected_t)
    for n, j in enumerate(order):
        arrived(a2[j])
        start_b1(j)
        projected_t = normed_block(3 + n, projected_t)
    projected_t = normed_block(6, projected_t)
    projected_t = normed_block(7, projected_t)
    up_term[...] = scale_factor * jnp.dot(
        projected_t.astype(BF16), v[...], preferred_element_type=F32
    )
    for n, j in enumerate(order):
        arrived(b1[j])
        start_b2(j)
        if n == 0:
            total = through_block(c, 0, total)
        if n == 1:
            across[0].wait_recv()
            total = through_block(1 - c, 0, total)
    last = None
    for j in order:
        arrived(b2[j])
        across[j] = links.send("c", 0, wbuf.at[c, j], wbuf.at[c, j])
        total = through_block(c, j, total)
        if last is not None:
            across[last].wait_recv()
            total = through_block(1 - c, last, total)
        last = j
    across[last].wait_recv()
    total = through_block(1 - c, last, total)

    drop = inverse * inverse * inverse * (total * (1.0 / 8192))
    stores = []
    for k in range(8):
        loads[k][1].wait()
        rows_out = rb[k].astype(F32) + inverse * gained[k] - xb[k].astype(F32) * drop
        rb[k] = rows_out.astype(BF16)
        store = pltpu.make_async_copy(rb.at[k], out.at[:, pl.ds(k * 1024, 1024)], out_sems.at[k])
        store.start()
        stores.append(store)
    for store in stores:
        store.wait()
    links.finish()


def main_block(scale_factor, hidden, resid, wsh, v, up, gain, down_t):
    dma = pltpu.SemaphoreType.DMA
    return pl.pallas_call(
        functools.partial(main_kernel, scale_factor),
        out_shape=(
            jax.ShapeDtypeStruct((256, 8192), BF16),
            jax.ShapeDtypeStruct((8, 16, 1024), F32),
            jax.ShapeDtypeStruct((16, 1024), F32),
        ),
        in_specs=[ANY, ANY, ANY, VMEM, VMEM, VMEM, VMEM],
        out_specs=(ANY, VMEM, VMEM),
        scratch_shapes=[
            pltpu.VMEM((2, 4, 1024, 1024), BF16),
            pltpu.VMEM((8, 256, 1024), BF16),
            pltpu.VMEM((8, 256, 1024), BF16),
            pltpu.VMEM((8, 256, 1024), F32),
            dma((64,)), dma((64,)), dma((17,)), dma((8,)),
        ],
        compiler_params=pltpu.CompilerParams(
            collective_id=1, has_side_effects=True, vmem_limit_bytes=60 * 1024 * 1024
        ),
        name="main_block",
    )(hidden, resid, wsh, v, up, gain, down_t)


def chunked(count, act):
    def step(i, carry):
        act(pl.ds(pl.multiple_of(i * 16, 16), 16))
        return carry

    lax.fori_loop(0, count // 16, step, 0)


class RingSum:
    def __init__(self, links, axis, blocks, relay, mid, near):
        self.links, self.axis, self.blocks = links, axis, blocks
        self.relay, self.mid, self.near = relay, mid, near
        m = links.x if axis == "x" else links.y if axis == "y" else links.z
        self.me, self.count = m, blocks.shape[2]

    def start(self):
        send, b, axis = self.links.send, self.blocks, self.axis
        far = wrap(self.me + 2, 4)
        right, left = wrap(self.me + 1, 4), wrap(self.me - 1, 4)
        self.far = [
            send(axis, 1, b.at[far, 0], self.relay.at[0]),
            send(axis, -1, b.at[far, 1], self.relay.at[1]),
        ]
        self.direct = [
            send(axis, 1, b.at[right, 1], self.near.at[0, 1]),
            send(axis, -1, b.at[left, 0], self.near.at[1, 0]),
        ]

    def forward(self):
        for way, step in ((0, 1), (1, -1)):
            self.far[way].wait_recv()
            to = wrap(self.me + step, 4)

            def add(span, way=way, to=to):
                self.mid[way, span] = (
                    self.blocks[to, way, span].astype(F32) + self.relay[way, span].astype(F32)
                ).astype(BF16)

            chunked(self.count, add)
            self.direct.append(
                self.links.send(self.axis, step, self.mid.at[way], self.near.at[way, way])
            )

    def finish(self, put):
        for copy in self.direct:
            copy.wait_recv()
        for half in range(2):

            def add(span, half=half):
                put(
                    half,
                    span,
                    self.blocks[self.me, half, span].astype(F32)
                    + self.near[0, half, span].astype(F32)
                    + self.near[1, half, span].astype(F32),
                )

            chunked(self.count, add)


def owner_kernel(
    qa, qb, outa, outb,
    relay_a, mid_a, near_a, next_a, relay_b, mid_b, near_b, next_b,
    relay_c, mid_c, near_c, relay_d, mid_d, near_d,
    send_sems, recv_sems,
):
    links = Links(send_sems, recv_sems)
    links.meet([("y", 1), ("y", -1), ("z", 1), ("z", -1)])
    sum_a = RingSum(links, "z", qa, relay_a, mid_a, near_a)
    sum_b = RingSum(links, "y", qb, relay_b, mid_b, near_b)
    sum_a.start()
    sum_b.start()
    sum_a.forward()
    sum_b.forward()

    def into(ref):
        def put(half, span, value):
            i = span.start // 16
            ref[2 * half + i // 2, lax.rem(i, 2)] = value.astype(BF16)

        return put

    sum_a.finish(into(next_a))
    sum_c = RingSum(links, "y", next_a, relay_c, mid_c, near_c)
    sum_c.start()
    sum_b.finish(into(next_b))
    sum_d = RingSum(links, "z", next_b, relay_d, mid_d, near_d)
    sum_d.start()
    sum_c.forward()
    sum_d.forward()

    def result(ref):
        def put(half, span, value):
            ref[half] = value

        return put

    sum_c.finish(result(outa))
    sum_d.finish(result(outb))
    links.finish()


def to_owners(qa, qb):
    wa, wb = qa.shape[-1], qb.shape[-1]
    dma = pltpu.SemaphoreType.DMA

    def big(w):
        return [
            pltpu.VMEM((2, 64, w), BF16),
            pltpu.VMEM((2, 64, w), BF16),
            pltpu.VMEM((2, 2, 64, w), BF16),
            pltpu.VMEM((4, 2, 16, w), BF16),
        ]

    def small(w):
        return [
            pltpu.VMEM((2, 16, w), BF16),
            pltpu.VMEM((2, 16, w), BF16),
            pltpu.VMEM((2, 2, 16, w), BF16),
        ]

    return pl.pallas_call(
        owner_kernel,
        out_shape=(
            jax.ShapeDtypeStruct((2, 16, wa), F32),
            jax.ShapeDtypeStruct((2, 16, wb), F32),
        ),
        in_specs=[VMEM, VMEM],
        out_specs=(VMEM, VMEM),
        scratch_shapes=big(wa) + big(wb) + small(wa) + small(wb) + [dma((24,)), dma((24,))],
        compiler_params=pltpu.CompilerParams(collective_id=2, has_side_effects=True),
        name="to_owners",
    )(qa, qb)


def sum_kernel(
    part, mpart, out, mout,
    half_in, ay, ry, bxz, rxz, gy, gc, mr,
    send_sems, recv_sems,
):
    links = Links(send_sems, recv_sems)
    x, y, z, c = links.x, links.y, links.z, links.c
    m16 = x * 4 + z

    def plane(k):
        d = lax.rem(m16 + k, 16)
        return {"dp": d // 4, "enc": lax.rem(d, 4)}

    barrier = pltpu.get_barrier_semaphore()
    peers = [links.peer("y", 1), links.peer("y", 2), links.peer("y", 3), links.peer("c", 0)]
    peers += [plane(k) for k in range(1, 16)]
    for peer in peers:
        pl.semaphore_signal(barrier, inc=1, device_id=peer, device_id_type=MESH)
    pl.semaphore_wait(barrier, len(peers))

    msum = [links.send("x", k, mpart, mr.at[k - 1]) for k in (1, 2, 3)]
    other = pl.ds(pl.multiple_of((1 - c) * 8, 8), 8)
    mine = pl.ds(pl.multiple_of(c * 8, 8), 8)
    swap = links.send("c", 0, part.at[other], half_in)
    swap.wait_recv()
    for b in range(4):
        cols = slice(b * 4096, (b + 1) * 4096)
        ay[b] = part[mine, cols] + half_in[:, cols]
    along = [links.send("y", k, ay.at[wrap(y + k, 4)], ry.at[k - 1]) for k in (1, 2, 3)]
    for copy in along:
        copy.wait_recv()
    mine_y = ay.at[y]
    for b in range(16):
        cols = slice(b * 256, (b + 1) * 256)
        bxz[b] = (mine_y[:, cols] + ry[0, :, cols]) + (ry[1, :, cols] + ry[2, :, cols])
    base = len(links.made)

    def spread(k):
        return pltpu.make_async_remote_copy(
            src_ref=bxz.at[lax.rem(m16 + k, 16)], dst_ref=rxz.at[k], send_sem=send_sems.at[base + k],
            recv_sem=recv_sems.at[base + k], device_id=plane(k), device_id_type=MESH,
        )

    def share(k, slot):
        return pltpu.make_async_remote_copy(
            src_ref=gy.at[y, m16], dst_ref=gy.at[y, slot], send_sem=send_sems.at[base + 16 + k],
            recv_sem=recv_sems.at[base + 16 + k], device_id=plane(k), device_id_type=MESH,
        )

    def over(act):
        def step(k, carry):
            act(k)
            return carry

        lax.fori_loop(1, 16, step, 0)

    over(lambda k: spread(k).start())
    over(lambda k: spread(k).wait_recv())
    rxz[0] = bxz[m16]
    value = rxz[0]
    for k in range(1, 16):
        value = value + rxz[k]
    gy[y, m16] = value
    over(lambda k: share(k, m16).start())
    for copy in msum:
        copy.wait_recv()
    mout[...] = (mpart[...] + mr[0]) + (mr[1] + mr[2])
    over(lambda k: share(k, lax.rem(m16 - k + 16, 16)).wait_recv())
    links.made += [None] * 32
    wide = [links.send("y", k, gy.at[y], gy.at[y]) for k in (1, 2, 3)]
    for copy in wide:
        copy.wait_recv()
    last = links.send("c", 0, gy, gc)
    for b in range(64):
        out[mine, b * 256 : (b + 1) * 256] = gy[b // 16, b % 16]
    last.wait_recv()
    for b in range(64):
        out[other, b * 256 : (b + 1) * 256] = gc[b // 16, b % 16]
    over(lambda k: spread(k).wait_send())
    over(lambda k: share(k, m16).wait_send())
    links.made = [copy for copy in links.made if copy is not None]
    links.finish()


def summed(part, mpart):
    dma = pltpu.SemaphoreType.DMA
    return pl.pallas_call(
        sum_kernel,
        out_shape=(
            jax.ShapeDtypeStruct(part.shape, F32),
            jax.ShapeDtypeStruct(mpart.shape, F32),
        ),
        in_specs=[VMEM, VMEM],
        out_specs=(VMEM, VMEM),
        scratch_shapes=[
            pltpu.VMEM((8, 16384), F32),
            pltpu.VMEM((4, 8, 4096), F32),
            pltpu.VMEM((3, 8, 4096), F32),
            pltpu.VMEM((16, 8, 256), F32),
            pltpu.VMEM((16, 8, 256), F32),
            pltpu.VMEM((4, 16, 8, 256), F32),
            pltpu.VMEM((4, 16, 8, 256), F32),
            pltpu.VMEM((3, 16, 256), F32),
            dma((48,)), dma((48,)),
        ],
        compiler_params=pltpu.CompilerParams(collective_id=3, has_side_effects=True),
        name="summed",
    )(part, mpart)


def gelu_parts(preact):
    normal_cdf = 0.5 * (1.0 + lax.erf(preact * 0.7071067811865476))
    normal_pdf = jnp.exp(-0.5 * preact * preact) * 0.3989422804014327
    return (normal_cdf, normal_pdf)


def owner_layout(image_token_counts, image_encoder_owner, owner_count, owner_room, slot_len):
    image_ids = jnp.arange(image_token_counts.shape[0])
    same_owner = image_encoder_owner[:, None] == image_encoder_owner[None, :]
    earlier = image_ids[None, :] < image_ids[:, None]
    starts = jnp.sum(jnp.where(same_owner & earlier, image_token_counts[None, :], 0), axis=1)
    row_index = jnp.arange(owner_count * owner_room)
    row_owner = row_index // owner_room
    row_place = row_index % owner_room
    matches = (
        (row_owner[:, None] == image_encoder_owner[None, :])
        & (row_place[:, None] >= starts[None, :])
        & (row_place[:, None] < (starts + image_token_counts)[None, :])
    )
    source = jnp.sum(
        jnp.where(matches, image_ids[None, :] * slot_len + row_place[:, None] - starts[None, :], 0),
        axis=1,
    )
    return jnp.where(jnp.any(matches, axis=1), source, -1)


def window(value, first):
    start = jnp.minimum(first, value.shape[0] - MAXIMG)
    rows = lax.dynamic_slice_in_dim(value, start, MAXIMG, 0)
    return lax.dynamic_slice_in_dim(jnp.concatenate([rows, rows], axis=0), first - start, MAXIMG, 0)


def body(
    hidden,
    residual_gradient,
    value_output_gradient,
    attention_norm_gain,
    value_frozen_weight,
    value_down_factor,
    value_up_factor,
    merger_frozen_weight,
    merger_down_factor,
    merger_up_factor,
    merger_saved_preactivation,
    image_token_counts,
    image_encoder_owner,
    image_first_rows,
):
    scale_factor = 256.0 / (hidden.shape[0] * 128) * adapter_scale
    x, y, z, c = place()
    member = (2 * y + c) * 4 + z
    gain = attention_norm_gain.reshape(8, 1, 1024)
    down_t = value_down_factor.T.reshape(16, 8, 1024).transpose(1, 0, 2)

    preact = merger_saved_preactivation.astype(F32)
    normal_cdf, normal_pdf = gelu_parts(preact)
    activation = (preact * normal_cdf).astype(BF16)
    act_low = jnp.dot(activation, merger_down_factor, preferred_element_type=F32).astype(BF16)
    act_low = jnp.pad(act_low, ((0, 0), (0, 112)))

    first = image_first_rows[0]
    count = lax.dynamic_index_in_dim(image_token_counts, member, 0, keepdims=False)
    keep = jnp.broadcast_to((jnp.arange(MAXIMG) < count)[:, None], (MAXIMG, 128)).astype(F32)
    vrecv, alow, wm_other, mup_other = image_chain(
        window(value_output_gradient, first),
        window(hidden, first),
        window(residual_gradient, first),
        keep,
        gain,
        value_frozen_weight,
        value_up_factor,
        down_t,
        act_low,
        merger_frozen_weight,
        merger_up_factor,
    )

    source = owner_layout(image_token_counts, image_encoder_owner, 32, 32, MAXIMG)
    mine = lax.dynamic_index_in_dim(source.reshape(4, 2, 4, 32), c, 1, keepdims=False)
    slots = jnp.arange(512)
    pick = (mine.reshape(512)[:, None] == slots[None, :]).astype(BF16)
    vis_own = lax.dynamic_index_in_dim(vrecv, c, 1, keepdims=False).reshape(512, 256)
    vis_other = lax.dynamic_index_in_dim(vrecv, 1 - c, 1, keepdims=False).reshape(512, 256)
    rows_own = jnp.dot(pick, vis_own, preferred_element_type=F32).astype(BF16)
    rows_other = jnp.dot(pick, vis_other, preferred_element_type=F32).astype(BF16)
    low_part = dot_nt(rows_own, merger_up_factor) + dot_nt(rows_other, mup_other)
    partial = (
        dot_nt(rows_own, merger_frozen_weight)
        + dot_nt(rows_other, wm_other)
        + adapter_scale * jnp.dot(low_part, merger_down_factor.astype(F32).T)
    ).astype(BF16)
    cut = 2560
    qa = partial[:, :cut].reshape(4, 4, 32, cut).transpose(1, 0, 2, 3).reshape(4, 2, 64, cut)
    qb = jnp.concatenate(
        [partial[:, cut:], jnp.pad(low_part, ((0, 0), (0, 112))).astype(BF16)], axis=1
    ).reshape(4, 2, 64, cut + 128)

    pick_all = (source[:, None] == slots[None, :]).astype(BF16)
    low_slots = dot_tn(pick_all, alow[:, :, :16].reshape(1024, 16)).astype(BF16)
    term_b2 = scale_factor * dot_tn(low_slots, vis_own)

    layer_input_gradient, down_term, up_term = main_block(
        scale_factor,
        hidden,
        residual_gradient,
        value_frozen_weight,
        value_output_gradient,
        value_up_factor,
        gain,
        down_t,
    )
    outa, outb = to_owners(qa, qb)
    combined = jnp.concatenate(
        [outa.reshape(32, cut), outb.reshape(32, cut + 128)[:, :cut]], axis=1
    )
    low_sum = outb.reshape(32, cut + 128)[:, cut : cut + 16]
    preactivation_gradient = (combined * (normal_cdf + preact * normal_pdf)).astype(BF16)
    term_a2 = scale_factor * dot_tn(low_sum.astype(BF16), activation)
    part = jnp.concatenate(
        [
            down_term.transpose(1, 0, 2).reshape(16, 8192),
            up_term,
            term_a2,
            jnp.zeros((16, 2048), F32),
        ],
        axis=1,
    )
    sums, merger_up_gradient = summed(part, term_b2)
    return (
        layer_input_gradient,
        preactivation_gradient,
        sums[:, :8192].T,
        sums[:, 8192:9216],
        sums[:, 9216:14336].T,
        merger_up_gradient,
    )


def solution(mesh):
    tokens = P(("dp", "fsdp", "enc"), None)
    features = P(None, ("fsdp", "enc"))
    placed = (
        tokens,
        tokens,
        tokens,
        P(),
        P("fsdp", None),
        P(),
        P(),
        features,
        P(),
        features,
        tokens,
        P("dp"),
        P("dp"),
        P(("dp", "fsdp", "enc")),
    )
    return jax.shard_map(
        body,
        mesh=mesh,
        in_specs=placed,
        out_specs=(tokens, tokens, P(), P(), P(), features),
        check_vma=False,
    )
```

```python
import functools

import jax
import jax.numpy as jnp
from jax import lax
from jax.experimental import pallas as pl
from jax.experimental.pallas import tpu as pltpu
from jax.sharding import PartitionSpec as P

MAXIMG = 16
adapter_scale = 2.0
norm_eps = 1e-06
F32, BF16 = jnp.float32, jnp.bfloat16
MESH = pl.DeviceIdType.MESH
VMEM = pl.BlockSpec(memory_space=pltpu.VMEM)
ANY = pl.BlockSpec(memory_space=pl.ANY)


def dot_nt(a, b):
    return lax.dot_general(a, b, (((1,), (1,)), ((), ())), preferred_element_type=F32)


def dot_tn(a, b):
    return lax.dot_general(a, b, (((0,), (0,)), ((), ())), preferred_element_type=F32)


def wrap(v, n):
    return lax.rem(v + n, n)


def place():
    f = lax.axis_index("fsdp")
    return lax.axis_index("dp"), f // 2, lax.axis_index("enc"), lax.rem(f, 2)


class Links:
    def __init__(self, send_sems, recv_sems):
        self.x, self.y, self.z, self.c = place()
        self.send_sems, self.recv_sems = send_sems, recv_sems
        self.made = []

    def peer(self, axis, step):
        if axis == "x":
            return {"dp": wrap(self.x + step, 4)}
        if axis == "z":
            return {"enc": wrap(self.z + step, 4)}
        if axis == "y":
            return {"fsdp": 2 * wrap(self.y + step, 4) + self.c}
        return {"fsdp": 2 * self.y + 1 - self.c}

    def send(self, axis, step, src, dst):
        k = len(self.made)
        copy = pltpu.make_async_remote_copy(
            src_ref=src,
            dst_ref=dst,
            send_sem=self.send_sems.at[k],
            recv_sem=self.recv_sems.at[k],
            device_id=self.peer(axis, step),
            device_id_type=MESH,
        )
        copy.start()
        self.made.append(copy)
        return copy

    def finish(self):
        for copy in self.made:
            copy.wait_send()

    def meet(self, peers):
        barrier = pltpu.get_barrier_semaphore()
        for axis, step in peers:
            pl.semaphore_signal(barrier, inc=1, device_id=self.peer(axis, step), device_id_type=MESH)
        pl.semaphore_wait(barrier, len(peers))


def chunked(count, act):
    def step(i, carry):
        act(pl.ds(pl.multiple_of(i * 16, 16), 16))
        return carry

    lax.fori_loop(0, count // 16, step, 0)


class RingSum:
    def __init__(self, links, axis, blocks, relay, mid, near):
        self.links, self.axis, self.blocks = links, axis, blocks
        self.relay, self.mid, self.near = relay, mid, near
        m = links.x if axis == "x" else links.y if axis == "y" else links.z
        self.me, self.count = m, blocks.shape[2]

    def start(self):
        send, b, axis = self.links.send, self.blocks, self.axis
        far = wrap(self.me + 2, 4)
        right, left = wrap(self.me + 1, 4), wrap(self.me - 1, 4)
        self.far = [
            send(axis, 1, b.at[far, 0], self.relay.at[0]),
            send(axis, -1, b.at[far, 1], self.relay.at[1]),
        ]
        self.direct = [
            send(axis, 1, b.at[right, 1], self.near.at[0, 1]),
            send(axis, -1, b.at[left, 0], self.near.at[1, 0]),
        ]

    def forward(self):
        for way, step in ((0, 1), (1, -1)):
            self.far[way].wait_recv()
            to = wrap(self.me + step, 4)

            def add(span, way=way, to=to):
                self.mid[way, span] = (
                    self.blocks[to, way, span].astype(F32) + self.relay[way, span].astype(F32)
                ).astype(BF16)

            chunked(self.count, add)
            self.direct.append(
                self.links.send(self.axis, step, self.mid.at[way], self.near.at[way, way])
            )

    def finish(self, put):
        for copy in self.direct:
            copy.wait_recv()
        for half in range(2):

            def add(span, half=half):
                put(
                    half,
                    span,
                    self.blocks[self.me, half, span].astype(F32)
                    + self.near[0, half, span].astype(F32)
                    + self.near[1, half, span].astype(F32),
                )

            chunked(self.count, add)


class AdapterSum:
    def __init__(self, links, src, out, bufs, sems):
        self.links, self.src, self.out = links, src, out
        self.half_in, self.ay, self.ry, self.bxz, self.rxz, self.gy, self.gc = bufs
        self.sems = sems
        self.m16 = links.x * 4 + links.z
        self.other = pl.ds(pl.multiple_of((1 - links.c) * 8, 8), 8)
        self.mine = pl.ds(pl.multiple_of(links.c * 8, 8), 8)

    def plane(self, k):
        d = lax.rem(self.m16 + k, 16)
        return {"dp": d // 4, "enc": lax.rem(d, 4)}

    def spread(self, k):
        return pltpu.make_async_remote_copy(
            src_ref=self.bxz.at[lax.rem(self.m16 + k, 16)], dst_ref=self.rxz.at[k],
            send_sem=self.sems[0].at[k], recv_sem=self.sems[1].at[k],
            device_id=self.plane(k), device_id_type=MESH,
        )

    def share(self, k, slot):
        return pltpu.make_async_remote_copy(
            src_ref=self.gy.at[self.links.y, self.m16], dst_ref=self.gy.at[self.links.y, slot],
            send_sem=self.sems[2].at[k], recv_sem=self.sems[3].at[k],
            device_id=self.plane(k), device_id_type=MESH,
        )

    def swap(self):
        self.swapped = self.links.send("c", 0, self.src.at[self.other], self.half_in)

    def along(self):
        self.swapped.wait_recv()
        for b in range(4):
            cols = slice(b * 2048, (b + 1) * 2048)
            self.ay[b] = self.src[self.mine, cols] + self.half_in[:, cols]
        y = self.links.y
        self.sent = [
            self.links.send("y", k, self.ay.at[wrap(y + k, 4)], self.ry.at[k - 1]) for k in (1, 2, 3)
        ]

    def across(self):
        for copy in self.sent:
            copy.wait_recv()
        here = self.ay.at[self.links.y]
        for b in range(16):
            cols = slice(b * 128, (b + 1) * 128)
            self.bxz[b] = (here[:, cols] + self.ry[0, :, cols]) + (
                self.ry[1, :, cols] + self.ry[2, :, cols]
            )
        over(1, 16, lambda k: self.spread(k).start())

    def back(self):
        over(1, 16, lambda k: self.spread(k).wait_recv())
        value = self.bxz[self.m16]
        for k in range(1, 16):
            value = value + self.rxz[k]
        self.gy[self.links.y, self.m16] = value
        over(1, 16, lambda k: self.share(k, self.m16).start())

    def outward(self):
        over(1, 16, lambda k: self.share(k, lax.rem(self.m16 - k + 16, 16)).wait_recv())
        y = self.links.y
        self.wide = [self.links.send("y", k, self.gy.at[y], self.gy.at[y]) for k in (1, 2, 3)]

    def last(self):
        for copy in self.wide:
            copy.wait_recv()
        self.final = self.links.send("c", 0, self.gy, self.gc)
        for b in range(64):
            self.out[self.mine, b * 128 : (b + 1) * 128] = self.gy[b // 16, b % 16]

    def end(self):
        self.final.wait_recv()
        for b in range(64):
            self.out[self.other, b * 128 : (b + 1) * 128] = self.gc[b // 16, b % 16]
        over(1, 16, lambda k: self.spread(k).wait_send())
        over(1, 16, lambda k: self.share(k, self.m16).wait_send())


def over(lo, hi, act):
    def step(j, carry):
        act(j)
        return carry

    lax.fori_loop(lo, hi, step, 0)


def big_kernel(
    scale_factor,
    first_row, counts_s, counts, owners, v, up, gain, down_t, preact, md, mup,
    hidden, resid, wsh, wm,
    through_out, low_out_ref, inverse_out, drop_out, outa, outb, sums1, sums2, mout,
    wbuf, xb, rb, through, send_sems, recv_sems, local_sems, out_sems,
    vimg, xsel, rsel, vall, tout, timg, gained, visout, vrecv, actl, alow, act,
    s1, r1, s2, r2, s3, r3, s4, r4,
    wmb, mup_other, lowp, lowin, s5, r5, rows_own, rows_other, mpart, mr,
    qa, qb,
    relay_a, mid_a, near_a, next_a, relay_b, mid_b, near_b, next_b,
    relay_c, mid_c, near_c, relay_d, mid_d, near_d,
    part1, part2, *rest,
):
    bufs1, bufs2, sems1, sems2 = rest[:7], rest[7:14], rest[14:18], rest[18:22]
    links = Links(send_sems, recv_sems)
    x, y, z, c = links.x, links.y, links.z, links.c
    f = 2 * y + c
    me = f * 4 + z

    own = pltpu.make_async_copy(wsh, wbuf.at[c, 0], local_sems.at[0])
    own.start()
    loads = []
    for k in range(8):
        cols = pl.ds(k * 1024, 1024)
        a = pltpu.make_async_copy(hidden.at[:, cols], xb.at[k], local_sems.at[1 + k])
        b = pltpu.make_async_copy(resid.at[:, cols], rb.at[k], local_sems.at[9 + k])
        a.start()
        b.start()
        loads.append((a, b))
    wm_load = pltpu.make_async_copy(wm, wmb.at[0], local_sems.at[17])
    wm_load.start()

    barrier = pltpu.get_barrier_semaphore()

    def plane_peer(j):
        d = lax.rem(me + j, 32)
        return {"fsdp": d // 4, "enc": lax.rem(d, 4)}

    def greet(j):
        pl.semaphore_signal(barrier, inc=1, device_id=plane_peer(j), device_id_type=MESH)

    def greet_x(j):
        d = 4 + j
        pl.semaphore_signal(
            barrier,
            inc=1,
            device_id={"dp": lax.rem(x + d // 4, 4), "enc": lax.rem(z + d, 4)},
            device_id_type=MESH,
        )

    over(1, 32, greet)
    over(0, 12, greet_x)
    first = first_row[0]
    lane = lax.broadcasted_iota(jnp.int32, (16, 256), 1)
    line = lax.broadcasted_iota(jnp.int32, (16, 256), 0)
    sel = jnp.where(lane == line + first, 1.0, 0.0).astype(BF16)
    vimg[...] = jnp.dot(sel, v[...], preferred_element_type=F32).astype(BF16)
    pl.semaphore_wait(barrier, 43)

    def row(j, slot):
        return pltpu.make_async_remote_copy(
            src_ref=vimg, dst_ref=vall.at[slot], send_sem=s1.at[j], recv_sem=r1.at[j],
            device_id={"fsdp": lax.rem(f + j, 8)}, device_id_type=MESH,
        )

    def back(j, slot):
        return pltpu.make_async_remote_copy(
            src_ref=tout.at[lax.rem(f + j, 8)], dst_ref=timg.at[slot], send_sem=s2.at[j],
            recv_sem=r2.at[j], device_id={"fsdp": lax.rem(f + j, 8)}, device_id_type=MESH,
        )

    def spread(j, slot):
        d = lax.rem(me + j, 32)
        return pltpu.make_async_remote_copy(
            src_ref=visout.at[d // 8, lax.rem(d, 4)], dst_ref=vrecv.at[slot], send_sem=s3.at[j],
            recv_sem=r3.at[j], device_id=plane_peer(j), device_id_type=MESH,
        )

    def low_out(j, slot):
        return pltpu.make_async_remote_copy(
            src_ref=actl, dst_ref=alow.at[slot], send_sem=s4.at[j], recv_sem=r4.at[j],
            device_id=plane_peer(j), device_id_type=MESH,
        )

    my16 = y * 4 + z

    def low_row(j, slot):
        d = lax.rem(my16 + j, 16)
        return pltpu.make_async_remote_copy(
            src_ref=lowp.at[d], dst_ref=lowin.at[slot], send_sem=s5.at[j], recv_sem=r5.at[j],
            device_id={"fsdp": 2 * (d // 4) + c, "enc": lax.rem(d, 4)}, device_id_type=MESH,
        )

    def at(j, start, count):
        return wbuf.at[c, j, pl.ds(pl.multiple_of(start, 16), count)]

    def piece(step):
        return (x * 4 + wrap(z + step, 4)) * 64

    def block(step):
        return wrap(x + step, 4) * 256

    moved = {}

    def arrived(name):
        for copy in moved[name]:
            copy.wait_recv()

    def start_y1():
        src = at(0, piece(0), 64)
        moved["y1"] = [
            links.send("y", 1, src, at(3, piece(0), 64)),
            links.send("y", -1, src, at(1, piece(0), 64)),
        ]

    def start_y2():
        moved["y2"] = [
            links.send("y", 1, at(3, piece(0), 32), at(2, piece(0), 32)),
            links.send("y", -1, at(1, piece(0) + 32, 32), at(2, piece(0) + 32, 32)),
        ]

    def start_a1(j):
        here = at(j, piece(0), 64)
        moved["a1", j] = [links.send("z", step, here, here) for step in (1, -1)]

    def start_a2(j):
        one, two = at(j, piece(-1), 32), at(j, piece(1) + 32, 32)
        moved["a2", j] = [links.send("z", 1, one, one), links.send("z", -1, two, two)]

    def start_b1(j):
        here = at(j, block(0), 256)
        moved["b1", j] = [links.send("x", step, here, here) for step in (1, -1)]

    def start_b2(j):
        one, two = at(j, block(-1), 128), at(j, block(1) + 128, 128)
        moved["b2", j] = [links.send("x", 1, one, one), links.send("x", -1, two, two)]

    def start_core(j):
        moved["core", j] = [links.send("c", 0, wbuf.at[c, j], wbuf.at[c, j])]

    over(1, 8, lambda j: row(j, f).start())
    own.wait()
    start_y1()
    wide = links.send("c", 0, wm, wmb.at[1])
    thin = links.send("c", 0, mup, mup_other)
    start_core(0)
    vall[f] = vimg[...]

    low_img = dot_nt(vimg[...], up[...]).astype(BF16)
    squares_img = jnp.zeros((16, 1), F32)
    for k in range(8):
        loads[k][0].wait()
        rows = jnp.dot(sel, xb[k], preferred_element_type=F32)
        xsel[k] = rows.astype(BF16)
        squares_img = squares_img + jnp.sum(rows * rows, axis=1, keepdims=True)
    inverse_img = lax.rsqrt(squares_img * (1.0 / 8192) + norm_eps)

    over(1, 8, lambda j: row(j, lax.rem(f - j + 8, 8)).wait_recv())
    tout[...] = dot_nt(vall[...].reshape(128, 1024), wbuf[c, 0]).astype(BF16).reshape(8, 16, 1024)
    over(1, 8, lambda j: back(j, f).start())
    timg[f] = tout[f]
    arrived("y1")
    start_y2()
    start_a1(3)
    start_a1(1)

    for k in range(8):
        loads[k][1].wait()
        rsel[k] = jnp.dot(sel, rb[k], preferred_element_type=F32).astype(BF16)
    squares = jnp.zeros((256, 1), F32)
    for k in range(8):
        xs = xb[k].astype(F32)
        squares = squares + jnp.sum(xs * xs, axis=1, keepdims=True)
    inverse = lax.rsqrt(squares * (1.0 / 8192) + norm_eps)

    over(1, 8, lambda j: back(j, lax.rem(f - j + 8, 8)).wait_recv())
    total_img = jnp.zeros((16, 1), F32)
    for k in range(8):
        grad = timg[k].astype(F32) + adapter_scale * jnp.dot(
            low_img, down_t[k], preferred_element_type=F32
        )
        g = gain[k] * grad
        gained[k] = g
        total_img = total_img + jnp.sum(xsel[k].astype(F32) * g, axis=1, keepdims=True)
    drop_img = inverse_img * inverse_img * inverse_img * (total_img * (1.0 / 8192))
    inside = lax.broadcasted_iota(jnp.int32, (16, 1024), 0) < counts_s[me]
    for k in range(8):
        rows = (
            rsel[k].astype(F32) + inverse_img * gained[k] - xsel[k].astype(F32) * drop_img
        )
        rows = jnp.where(inside, rows, 0.0).astype(BF16)
        for b in range(4):
            visout[k // 2, b, k % 2] = rows[:, b * 256 : (b + 1) * 256]
    over(1, 32, lambda j: spread(j, me).start())
    vrecv[me] = visout[y, z]

    p = preact[...].astype(F32)
    act[...] = (p * (0.5 * (1.0 + lax.erf(p * 0.7071067811865476)))).astype(BF16)
    actl[...] = jnp.zeros_like(actl)
    actl[:, 0:16] = dot_nt(act[...], md[...]).astype(BF16)
    over(1, 32, lambda j: low_out(j, me).start())
    alow[me] = actl[...]

    arrived("y2")
    start_a1(2)
    arrived(("a1", 3))
    start_a2(3)
    arrived(("a1", 1))
    start_a2(1)

    low = dot_nt(v[...], up[...]).astype(BF16)
    low_out_ref[...] = low
    low_t = dot_nt(up[...], v[...]).astype(BF16)
    projected_t = jnp.zeros((16, 256), F32)
    for k in range(8):
        normed = (xb[k].astype(F32) * inverse * gain[k]).astype(BF16)
        part1[:, k * 1024 : (k + 1) * 1024] = scale_factor * jnp.dot(
            low_t, normed, preferred_element_type=F32
        )
        projected_t = projected_t + dot_nt(down_t[k], normed)
    sum1 = AdapterSum(links, part1, sums1, bufs1, sems1)
    sum1.swap()
    arrived(("a2", 3))
    start_b1(3)
    arrived(("a1", 2))
    start_a2(2)
    arrived(("a2", 1))
    start_b1(1)
    part2[:, 0:1024] = scale_factor * jnp.dot(
        projected_t.astype(BF16), v[...], preferred_element_type=F32
    )
    part2[:, 6144:8192] = jnp.zeros((16, 2048), F32)
    sum1.along()

    eye = lax.broadcasted_iota(jnp.int32, (32, 32), 0) == lax.broadcasted_iota(
        jnp.int32, (32, 32), 1
    )
    earlier = lax.broadcasted_iota(jnp.int32, (32, 32), 1) < lax.broadcasted_iota(
        jnp.int32, (32, 32), 0
    )
    counts_f = counts[...].astype(F32)
    owners_f = owners[...].astype(F32)
    owner_col = jnp.sum(jnp.where(eye, owners_f, 0.0), axis=1, keepdims=True)
    count_col = jnp.sum(jnp.where(eye, counts_f, 0.0), axis=1, keepdims=True)
    start_col = jnp.sum(
        jnp.where((owner_col == owners_f) & earlier, counts_f, 0.0), axis=1, keepdims=True
    )
    slot = lax.broadcasted_iota(jnp.int32, (32, 512), 1)
    image = lax.broadcasted_iota(jnp.int32, (32, 512), 0)
    inner = (slot % 16).astype(F32)
    key = (
        jnp.sum(
            jnp.where(
                (slot // 16 == image) & (inner < count_col),
                owner_col * 32.0 + start_col + inner + 1.0,
                0.0,
            ),
            axis=0,
            keepdims=True,
        )
        - 1.0
    )

    over(1, 32, lambda j: spread(j, lax.rem(me - j + 32, 32)).wait_recv())
    wide.wait_recv()
    thin.wait_recv()
    wm_load.wait()
    r = lax.broadcasted_iota(jnp.int32, (512, 1), 0)
    row_id = ((2 * (r // 128) + c) * 4 + (r // 32) % 4) * 32 + r % 32
    pick = jnp.where(row_id.astype(F32) == key, 1.0, 0.0).astype(BF16)
    rows_own[...] = jnp.dot(
        pick, vrecv[:, c].reshape(512, 256), preferred_element_type=F32
    ).astype(BF16)
    rows_other[...] = jnp.dot(
        pick, vrecv[:, 1 - c].reshape(512, 256), preferred_element_type=F32
    ).astype(BF16)
    low_part = dot_nt(rows_own[...], mup[...]) + dot_nt(rows_other[...], mup_other[...])
    lowp[...] = jnp.zeros_like(lowp)
    lowp[:, :, 0:16] = low_part.reshape(16, 32, 16)
    over(1, 16, lambda j: low_row(j, my16).start())
    low_hi = low_part.astype(BF16)
    low_lo = (low_part - low_hi.astype(F32)).astype(BF16)

    def columns(n):
        cols = pl.ds(pl.multiple_of(n * 512, 512), 512)
        value = dot_nt(rows_own[...], wmb[0, cols]) + dot_nt(rows_other[...], wmb[1, cols])
        value = value + adapter_scale * (
            jnp.dot(low_hi, md[:, cols], preferred_element_type=F32)
            + jnp.dot(low_lo, md[:, cols], preferred_element_type=F32)
        )
        return value.astype(BF16)

    def fill_a(n):
        value = columns(n)
        cols = pl.ds(pl.multiple_of(n * 512, 512), 512)
        for yy in range(4):
            for zz in range(4):
                at_row = yy * 128 + zz * 32
                qa[zz, yy // 2, (yy % 2) * 32 : (yy % 2) * 32 + 32, cols] = value[
                    at_row : at_row + 32
                ]

    def fill_b(n):
        value = columns(n + 5)
        cols = pl.ds(pl.multiple_of(n * 512, 512), 512)
        qb[:, :, :, cols] = value.reshape(4, 2, 64, 512)

    sum_a = RingSum(links, "z", qa, relay_a, mid_a, near_a)
    sum_b = RingSum(links, "y", qb, relay_b, mid_b, near_b)
    over(0, 5, fill_a)
    sum_a.start()
    over(0, 5, fill_b)
    sum_b.start()

    total = jnp.zeros((256, 1), F32)
    stores = []

    def through_block(cs, j, total):
        k = 2 * lax.rem(y + j, 4) + cs
        value = dot_nt(v[...], wbuf[cs, j]).astype(BF16)
        through[k] = value
        store = pltpu.make_async_copy(through.at[k], through_out.at[k], out_sems.at[len(stores)])
        store.start()
        stores.append(store)
        grad = value.astype(F32) + adapter_scale * jnp.dot(
            low, down_t[k], preferred_element_type=F32
        )
        return total + jnp.sum(xb[k].astype(F32) * (gain[k] * grad), axis=1, keepdims=True)

    arrived(("a2", 2))
    start_b1(2)
    over(1, 16, lambda j: low_row(j, lax.rem(my16 - j + 16, 16)).wait_recv())
    lowin[my16] = lowp[my16]
    low_sum = lowin[0]
    for k in range(1, 16):
        low_sum = low_sum + lowin[k]
    low_sum_t = low_sum.T[0:16].astype(BF16)
    part2[:, 1024:6144] = scale_factor * jnp.dot(
        low_sum_t, act[...], preferred_element_type=F32
    )
    sum2 = AdapterSum(links, part2, sums2, bufs2, sems2)
    sum2.swap()
    sum1.across()
    total = through_block(c, 0, total)
    sum2.along()
    sum_a.forward()
    sum_b.forward()
    arrived(("b1", 3))
    start_b2(3)
    arrived(("core", 0))
    total = through_block(1 - c, 0, total)
    sum1.back()

    over(1, 32, lambda j: low_out(j, lax.rem(me - j + 32, 32)).wait_recv())
    every = lax.broadcasted_iota(jnp.int32, (1024, 1), 0).astype(F32)
    pick_all = jnp.where(every == key, 1.0, 0.0).astype(BF16)
    low_slots = dot_tn(alow[...].reshape(1024, 128), pick_all).astype(BF16)
    mpart[...] = scale_factor * jnp.dot(
        low_slots[0:16], vrecv[:, c].reshape(512, 256), preferred_element_type=F32
    )
    msum = [links.send("x", k, mpart, mr.at[k - 1]) for k in (1, 2, 3)]
    sum2.across()
    arrived(("b1", 1))
    start_b2(1)
    sum1.outward()

    def into(ref):
        def put(half, span, value):
            i = span.start // 16
            ref[2 * half + i // 2, lax.rem(i, 2)] = value.astype(BF16)

        return put

    sum_a.finish(into(next_a))
    sum_c = RingSum(links, "y", next_a, relay_c, mid_c, near_c)
    sum_c.start()
    sum_b.finish(into(next_b))
    sum_d = RingSum(links, "z", next_b, relay_d, mid_d, near_d)
    sum_d.start()
    sum2.back()
    sum1.last()
    arrived(("b2", 3))
    start_core(3)
    total = through_block(c, 3, total)
    sum_c.forward()
    sum_d.forward()
    sum2.outward()
    arrived(("b1", 2))
    start_b2(2)
    arrived(("core", 3))
    total = through_block(1 - c, 3, total)
    for copy in msum:
        copy.wait_recv()
    mout[...] = (mpart[...] + mr[0]) + (mr[1] + mr[2])
    sum1.end()

    def result(ref):
        def put(half, span, value):
            ref[half] = value

        return put

    sum_c.finish(result(outa))
    sum_d.finish(result(outb))
    sum2.last()
    arrived(("b2", 1))
    start_core(1)
    total = through_block(c, 1, total)
    sum2.end()
    arrived(("core", 1))
    total = through_block(1 - c, 1, total)
    arrived(("b2", 2))
    start_core(2)
    total = through_block(c, 2, total)
    arrived(("core", 2))
    total = through_block(1 - c, 2, total)
    inverse_out[...] = inverse
    drop_out[...] = inverse * inverse * inverse * (total * (1.0 / 8192))

    for store in stores:
        store.wait()
    over(1, 8, lambda j: row(j, f).wait_send())
    over(1, 8, lambda j: back(j, f).wait_send())
    over(1, 32, lambda j: spread(j, me).wait_send())
    over(1, 32, lambda j: low_out(j, me).wait_send())
    over(1, 16, lambda j: low_row(j, my16).wait_send())
    links.finish()


def big_call(scale_factor, *args):
    dma = pltpu.SemaphoreType.DMA
    half = 2560

    def big(w):
        return [
            pltpu.VMEM((2, 64, w), BF16),
            pltpu.VMEM((2, 64, w), BF16),
            pltpu.VMEM((2, 2, 64, w), BF16),
            pltpu.VMEM((4, 2, 16, w), BF16),
        ]

    def small(w):
        return [
            pltpu.VMEM((2, 16, w), BF16),
            pltpu.VMEM((2, 16, w), BF16),
            pltpu.VMEM((2, 2, 16, w), BF16),
        ]

    def sums():
        return [
            pltpu.VMEM((8, 8192), F32),
            pltpu.VMEM((4, 8, 2048), F32),
            pltpu.VMEM((3, 8, 2048), F32),
            pltpu.VMEM((16, 8, 128), F32),
            pltpu.VMEM((16, 8, 128), F32),
            pltpu.VMEM((4, 16, 8, 128), F32),
            pltpu.VMEM((4, 16, 8, 128), F32),
        ]

    scalar = pl.BlockSpec(memory_space=pltpu.SMEM)
    shape = jax.ShapeDtypeStruct
    return pl.pallas_call(
        functools.partial(big_kernel, scale_factor),
        out_shape=(
            shape((8, 256, 1024), BF16),
            shape((256, 16), BF16),
            shape((256, 1), F32),
            shape((256, 1), F32),
            shape((2, 16, half), F32),
            shape((2, 16, half), F32),
            shape((16, 8192), F32),
            shape((16, 8192), F32),
            shape((16, 256), F32),
        ),
        in_specs=[scalar, scalar] + [VMEM] * 9 + [ANY] * 4,
        out_specs=(ANY,) + (VMEM,) * 8,
        scratch_shapes=[
            pltpu.VMEM((2, 4, 1024, 1024), BF16),
            pltpu.VMEM((8, 256, 1024), BF16),
            pltpu.VMEM((8, 256, 1024), BF16),
            pltpu.VMEM((8, 256, 1024), BF16),
            dma((96,)), dma((96,)), dma((18,)), dma((8,)),
            pltpu.VMEM((16, 1024), BF16),
            pltpu.VMEM((8, 16, 1024), BF16),
            pltpu.VMEM((8, 16, 1024), BF16),
            pltpu.VMEM((8, 16, 1024), BF16),
            pltpu.VMEM((8, 16, 1024), BF16),
            pltpu.VMEM((8, 16, 1024), BF16),
            pltpu.VMEM((8, 16, 1024), F32),
            pltpu.VMEM((4, 4, 2, 16, 256), BF16),
            pltpu.VMEM((32, 2, 16, 256), BF16),
            pltpu.VMEM((32, 128), BF16),
            pltpu.VMEM((32, 32, 128), BF16),
            pltpu.VMEM((32, 5120), BF16),
            dma((8,)), dma((8,)), dma((8,)), dma((8,)),
            dma((32,)), dma((32,)), dma((32,)), dma((32,)),
            pltpu.VMEM((2, 5120, 256), BF16),
            pltpu.VMEM((16, 256), BF16),
            pltpu.VMEM((16, 32, 128), F32),
            pltpu.VMEM((16, 32, 128), F32),
            dma((16,)), dma((16,)),
            pltpu.VMEM((512, 256), BF16),
            pltpu.VMEM((512, 256), BF16),
            pltpu.VMEM((16, 256), F32),
            pltpu.VMEM((3, 16, 256), F32),
            pltpu.VMEM((4, 2, 64, half), BF16),
            pltpu.VMEM((4, 2, 64, half), BF16),
            *big(half), *big(half), *small(half), *small(half),
            pltpu.VMEM((16, 8192), F32),
            pltpu.VMEM((16, 8192), F32),
            *sums(), *sums(),
            *[dma((16,)) for _ in range(8)],
        ],
        compiler_params=pltpu.CompilerParams(
            collective_id=0, has_side_effects=True, vmem_limit_bytes=67_043_328
        ),
        name="big",
    )(*args)


def finish_kernel(hidden, resid, through, gain, down_t, low, inverse, drop, out):
    grad = through[0].astype(F32) + adapter_scale * jnp.dot(
        low[...], down_t[0], preferred_element_type=F32
    )
    rows = (
        resid[...].astype(F32)
        + inverse[...] * (gain[0] * grad)
        - hidden[...].astype(F32) * drop[...]
    )
    out[...] = rows.astype(BF16)


def finish(hidden, resid, through, gain, down_t, low, inverse, drop):
    cols = pl.BlockSpec((256, 1024), lambda k: (0, k))

    def whole(shape):
        return pl.BlockSpec(shape, lambda k: (0, 0))

    def each(shape):
        return pl.BlockSpec((1, *shape), lambda k: (k, 0, 0))

    return pl.pallas_call(
        finish_kernel,
        grid=(8,),
        out_shape=jax.ShapeDtypeStruct((256, 8192), BF16),
        in_specs=[
            cols,
            cols,
            each((256, 1024)),
            each((1, 1024)),
            each((16, 1024)),
            whole((256, 16)),
            whole((256, 1)),
            whole((256, 1)),
        ],
        out_specs=cols,
        name="finish",
    )(hidden, resid, through, gain, down_t, low, inverse, drop)


def gelu_parts(preact):
    normal_cdf = 0.5 * (1.0 + lax.erf(preact * 0.7071067811865476))
    normal_pdf = jnp.exp(-0.5 * preact * preact) * 0.3989422804014327
    return (normal_cdf, normal_pdf)


def body(
    hidden,
    residual_gradient,
    value_output_gradient,
    attention_norm_gain,
    value_frozen_weight,
    value_down_factor,
    value_up_factor,
    merger_frozen_weight,
    merger_down_factor,
    merger_up_factor,
    merger_saved_preactivation,
    image_token_counts,
    image_encoder_owner,
    image_first_rows,
):
    scale_factor = 256.0 / (hidden.shape[0] * 128) * adapter_scale
    gain = attention_norm_gain.reshape(8, 1, 1024)
    down_t = value_down_factor.T.reshape(16, 8, 1024).transpose(1, 0, 2)
    through, low, inverse, drop, outa, outb, sums1, sums2, merger_up_gradient = big_call(
        scale_factor,
        image_first_rows,
        image_token_counts,
        image_token_counts.reshape(1, 32),
        image_encoder_owner.reshape(1, 32),
        value_output_gradient,
        value_up_factor,
        gain,
        down_t,
        merger_saved_preactivation,
        merger_down_factor.T,
        merger_up_factor,
        hidden,
        residual_gradient,
        value_frozen_weight,
        merger_frozen_weight,
    )
    layer_input_gradient = finish(
        hidden, residual_gradient, through, gain, down_t, low, inverse, drop
    )
    preact = merger_saved_preactivation.astype(F32)
    normal_cdf, normal_pdf = gelu_parts(preact)
    combined = jnp.concatenate([outa.reshape(32, 2560), outb.reshape(32, 2560)], axis=1)
    preactivation_gradient = (combined * (normal_cdf + preact * normal_pdf)).astype(BF16)
    return (
        layer_input_gradient,
        preactivation_gradient,
        sums1.T,
        sums2[:, :1024],
        sums2[:, 1024:6144].T,
        merger_up_gradient,
    )


def solution(mesh):
    tokens = P(("dp", "fsdp", "enc"), None)
    features = P(None, ("fsdp", "enc"))
    placed = (
        tokens,
        tokens,
        tokens,
        P(),
        P("fsdp", None),
        P(),
        P(),
        features,
        P(),
        features,
        tokens,
        P("dp"),
        P("dp"),
        P(("dp", "fsdp", "enc")),
    )
    return jax.shard_map(
        body,
        mesh=mesh,
        in_specs=placed,
        out_specs=(tokens, tokens, P(), P(), P(), features),
        check_vma=False,
    )
```

```python
import functools

import jax
import jax.numpy as jnp
from jax import lax
from jax.experimental import pallas as pl
from jax.experimental.pallas import tpu as pltpu
from jax.sharding import PartitionSpec as P

MAXIMG = 16
adapter_scale = 2.0
norm_eps = 1e-06
F32, BF16 = jnp.float32, jnp.bfloat16
MESH = pl.DeviceIdType.MESH
VMEM = pl.BlockSpec(memory_space=pltpu.VMEM)
ANY = pl.BlockSpec(memory_space=pl.ANY)


def dot_nt(a, b):
    return lax.dot_general(a, b, (((1,), (1,)), ((), ())), preferred_element_type=F32)


def dot_tn(a, b):
    return lax.dot_general(a, b, (((0,), (0,)), ((), ())), preferred_element_type=F32)


def wrap(v, n):
    return lax.rem(v + n, n)


def place():
    f = lax.axis_index("fsdp")
    return lax.axis_index("dp"), f // 2, lax.axis_index("enc"), lax.rem(f, 2)


class Links:
    def __init__(self, send_sems, recv_sems):
        self.x, self.y, self.z, self.c = place()
        self.send_sems, self.recv_sems = send_sems, recv_sems
        self.made = []
        self.taken = 0

    def peer(self, axis, step):
        if axis == "x":
            return {"dp": wrap(self.x + step, 4)}
        if axis == "z":
            return {"enc": wrap(self.z + step, 4)}
        if axis == "y":
            return {"fsdp": 2 * wrap(self.y + step, 4) + self.c}
        return {"fsdp": 2 * self.y + 1 - self.c}

    def take(self):
        self.taken += 1
        return self.send_sems.at[self.taken - 1], self.recv_sems.at[self.taken - 1]

    def send(self, axis, step, src, dst):
        return self.group([(axis, step, src, dst)], dst)

    def group(self, sends, whole):
        sems = self.take()
        for axis, step, src, dst in sends:
            self.copy(sems, src, dst, self.peer(axis, step)).start()
        total = self.copy(sems, whole, whole, self.peer(*sends[0][:2]))
        self.made.append(total)
        return total

    def copy(self, sems, src, dst, peer):
        return pltpu.make_async_remote_copy(
            src_ref=src,
            dst_ref=dst,
            send_sem=sems[0],
            recv_sem=sems[1],
            device_id=peer,
            device_id_type=MESH,
        )

    def finish(self):
        for copy in self.made:
            copy.wait_send()

    def meet(self, peers):
        barrier = pltpu.get_barrier_semaphore()
        for axis, step in peers:
            pl.semaphore_signal(barrier, inc=1, device_id=self.peer(axis, step), device_id_type=MESH)
        pl.semaphore_wait(barrier, len(peers))


def chunked(count, act):
    def step(i, carry):
        act(pl.ds(pl.multiple_of(i * 16, 16), 16))
        return carry

    lax.fori_loop(0, count // 16, step, 0)


class RingSum:
    def __init__(self, links, axis, blocks, relay, mid, near):
        self.links, self.axis, self.blocks = links, axis, blocks
        self.relay, self.mid, self.near = relay, mid, near
        m = links.x if axis == "x" else links.y if axis == "y" else links.z
        self.me, self.count = m, blocks.shape[2]

    def start(self):
        send, b, axis = self.links.send, self.blocks, self.axis
        far = wrap(self.me + 2, 4)
        right, left = wrap(self.me + 1, 4), wrap(self.me - 1, 4)
        self.far = [
            send(axis, 1, b.at[far, 0], self.relay.at[0]),
            send(axis, -1, b.at[far, 1], self.relay.at[1]),
        ]
        self.direct = [
            send(axis, 1, b.at[right, 1], self.near.at[0, 1]),
            send(axis, -1, b.at[left, 0], self.near.at[1, 0]),
        ]

    def forward(self):
        for way, step in ((0, 1), (1, -1)):
            self.far[way].wait_recv()
            to = wrap(self.me + step, 4)

            def add(span, way=way, to=to):
                self.mid[way, span] = (
                    self.blocks[to, way, span].astype(F32) + self.relay[way, span].astype(F32)
                ).astype(BF16)

            chunked(self.count, add)
            self.direct.append(
                self.links.send(self.axis, step, self.mid.at[way], self.near.at[way, way])
            )

    def finish(self, put):
        for copy in self.direct:
            copy.wait_recv()
        for half in range(2):

            def add(span, half=half):
                put(
                    half,
                    span,
                    self.blocks[self.me, half, span].astype(F32)
                    + self.near[0, half, span].astype(F32)
                    + self.near[1, half, span].astype(F32),
                )

            chunked(self.count, add)


class AdapterSum:
    def __init__(self, links, src, out, bufs):
        self.links, self.src, self.out = links, src, out
        self.half_in, self.ay, self.ry, self.bxz, self.rxz, self.gy, self.gc = bufs
        self.sems = links.take(), links.take()
        self.m16 = links.x * 4 + links.z
        self.other = pl.ds(pl.multiple_of((1 - links.c) * 8, 8), 8)
        self.mine = pl.ds(pl.multiple_of(links.c * 8, 8), 8)

    def plane(self, k):
        d = lax.rem(self.m16 + k, 16)
        return {"dp": d // 4, "enc": lax.rem(d, 4)}

    def spread(self, k):
        return self.links.copy(
            self.sems[0], self.bxz.at[lax.rem(self.m16 + k, 16)], self.rxz.at[k - 1], self.plane(k)
        )

    def share(self, k):
        here = self.gy.at[self.links.y, self.m16]
        return self.links.copy(self.sems[1], here, here, self.plane(k))

    def total(self, n):
        whole = self.rxz.at[0:15]
        return self.links.copy(self.sems[n], whole, whole, self.plane(1))

    def swap(self):
        self.swapped = self.links.send("c", 0, self.src.at[self.other], self.half_in)

    def along(self):
        self.swapped.wait_recv()
        for b in range(4):
            cols = slice(b * 2048, (b + 1) * 2048)
            self.ay[b] = self.src[self.mine, cols] + self.half_in[:, cols]
        y = self.links.y
        self.sent = self.links.group(
            [("y", k, self.ay.at[wrap(y + k, 4)], self.ry.at[k - 1]) for k in (1, 2, 3)], self.ry
        )

    def across(self):
        self.sent.wait_recv()
        here = self.ay.at[self.links.y]
        for b in range(16):
            cols = slice(b * 128, (b + 1) * 128)
            self.bxz[b] = (here[:, cols] + self.ry[0, :, cols]) + (
                self.ry[1, :, cols] + self.ry[2, :, cols]
            )
        over(1, 16, lambda k: self.spread(k).start())

    def back(self):
        self.total(0).wait_recv()
        value = self.bxz[self.m16]
        for k in range(15):
            value = value + self.rxz[k]
        self.gy[self.links.y, self.m16] = value
        over(1, 16, lambda k: self.share(k).start())

    def outward(self):
        self.total(1).wait_recv()
        here = self.gy.at[self.links.y]
        self.wide = self.links.group(
            [("y", k, here, here) for k in (1, 2, 3)], self.gy.at[0:3]
        )

    def last(self):
        self.wide.wait_recv()
        self.final = self.links.send("c", 0, self.gy, self.gc)
        for b in range(64):
            self.out[self.mine, b * 128 : (b + 1) * 128] = self.gy[b // 16, b % 16]

    def end(self):
        self.final.wait_recv()
        for b in range(64):
            self.out[self.other, b * 128 : (b + 1) * 128] = self.gc[b // 16, b % 16]
        self.total(0).wait_send()
        self.total(1).wait_send()


def over(lo, hi, act):
    def step(j, carry):
        act(j)
        return carry

    lax.fori_loop(lo, hi, step, 0)


def big_kernel(
    scale_factor,
    first_row, counts_s, counts, owners, up, mup,
    v_in, gain_in, down_in, preact_in, md_in, hidden, resid, wsh, wm,
    through_out, low_out_ref, inverse_out, drop_out, pgrad, sums1, sums2, mout,
    wbuf, xb, rb, through, send_sems, recv_sems, local_sems, out_sems,
    v, gain, down_t, preact, md, slope,
    vimg, xsel, rsel, vall, tout, timg, gained, visout, vrecv, actl, alow, act,
    wmb, mup_other, lowp, lowin, rows_own, rows_other, mpart, mr,
    qa, qb,
    relay_a, mid_a, near_a, next_a, relay_b, mid_b, near_b, next_b,
    relay_c, mid_c, near_c, relay_d, mid_d, near_d,
    part1, part2, *rest,
):
    bufs1, bufs2 = rest[:7], rest[7:14]
    links = Links(send_sems, recv_sems)
    x, y, z, c = links.x, links.y, links.z, links.c
    f = 2 * y + c
    me = f * 4 + z

    small = []
    pairs = ((v_in, v), (gain_in, gain), (down_in, down_t), (preact_in, preact), (md_in, md))
    for n, (src, dst) in enumerate(pairs):
        small.append(pltpu.make_async_copy(src, dst, local_sems.at[18 + n]))
        small[n].start()
    own = pltpu.make_async_copy(wsh, wbuf.at[c, 0], local_sems.at[0])
    own.start()
    loads = []
    for k in range(8):
        cols = pl.ds(k * 1024, 1024)
        a = pltpu.make_async_copy(hidden.at[:, cols], xb.at[k], local_sems.at[1 + k])
        b = pltpu.make_async_copy(resid.at[:, cols], rb.at[k], local_sems.at[9 + k])
        a.start()
        b.start()
        loads.append((a, b))
    wm_load = pltpu.make_async_copy(wm, wmb.at[0], local_sems.at[17])
    wm_load.start()

    barrier = pltpu.get_barrier_semaphore()

    def plane_peer(j):
        d = lax.rem(me + j, 32)
        return {"fsdp": d // 4, "enc": lax.rem(d, 4)}

    def greet(j):
        pl.semaphore_signal(barrier, inc=1, device_id=plane_peer(j), device_id_type=MESH)

    def greet_x(j):
        d = 4 + j
        pl.semaphore_signal(
            barrier,
            inc=1,
            device_id={"dp": lax.rem(x + d // 4, 4), "enc": lax.rem(z + d, 4)},
            device_id_type=MESH,
        )

    over(1, 32, greet)
    over(0, 12, greet_x)
    first = first_row[0]
    lane = lax.broadcasted_iota(jnp.int32, (16, 256), 1)
    line = lax.broadcasted_iota(jnp.int32, (16, 256), 0)
    sel = jnp.where(lane == line + first, 1.0, 0.0).astype(BF16)
    small[0].wait()
    vimg[...] = jnp.dot(sel, v[...], preferred_element_type=F32).astype(BF16)
    pl.semaphore_wait(barrier, 43)

    sems_row, sems_back, sems_spread = links.take(), links.take(), links.take()
    sems_low_out, sems_low_row = links.take(), links.take()
    my16 = y * 4 + z

    def row(j):
        return links.copy(sems_row, vimg, vall.at[f], {"fsdp": lax.rem(f + j, 8)})

    def back(j):
        to = lax.rem(f + j, 8)
        return links.copy(sems_back, tout.at[to], timg.at[f], {"fsdp": to})

    def spread(j):
        d = lax.rem(me + j, 32)
        return links.copy(sems_spread, visout.at[d // 8, lax.rem(d, 4)], vrecv.at[me], plane_peer(j))

    def low_out(j):
        return links.copy(sems_low_out, actl, alow.at[me], plane_peer(j))

    def low_row(j):
        d = lax.rem(my16 + j, 16)
        peer = {"fsdp": 2 * (d // 4) + c, "enc": lax.rem(d, 4)}
        return links.copy(sems_low_row, lowp.at[d], lowin.at[my16], peer)

    def all_of(sems, whole):
        return links.copy(sems, whole, whole, plane_peer(1))

    all_rows = all_of(sems_row, vall.at[0:7])
    all_back = all_of(sems_back, timg.at[0:7])
    all_spread = all_of(sems_spread, vrecv.at[0:31])
    all_low_out = all_of(sems_low_out, alow.at[0:31])
    all_low_rows = all_of(sems_low_row, lowin.at[0:15])

    def at(j, start, count):
        return wbuf.at[c, j, pl.ds(pl.multiple_of(start, 16), count)]

    def piece(step):
        return (x * 4 + wrap(z + step, 4)) * 48

    def block(step):
        return wrap(x + step, 4) * 192

    rest_at = 768
    moved = {}

    def arrived(name):
        moved[name].wait_recv()

    def group(name, rows, sends):
        moved[name] = links.group(sends, wbuf.at[c, 0, 0:rows])

    def start_y1():
        src = at(0, piece(0), 48)
        group("y1", 96, [("y", t, src, at(j, piece(0), 48)) for t, j in ((1, 3), (-1, 1))])

    def start_y2():
        sends = []
        for t, j, start, count in ((1, 3, piece(0), 32), (-1, 1, piece(0) + 32, 16)):
            sends.append(("y", t, at(j, start, count), at(2, start, count)))
        group("y2", 48, sends)

    def start_r1():
        src = at(0, rest_at, 256)
        group("r1", 512, [("y", t, src, at(j, rest_at, 256)) for t, j in ((1, 3), (-1, 1))])

    def start_r2():
        sends = []
        for t, j, start in ((1, 3, rest_at), (-1, 1, rest_at + 128)):
            sends.append(("y", t, at(j, start, 128), at(2, start, 128)))
        group("r2", 256, sends)

    def same(axis, step, j, start, count):
        here = at(j, start, count)
        return (axis, step, here, here)

    def start_a1(j):
        group(("a1", j), 96, [same("z", step, j, piece(0), 48) for step in (1, -1)])

    def start_a2(j):
        one = 32 if j == 3 else 16
        group(
            ("a2", j),
            48,
            [same("z", 1, j, piece(-1), one), same("z", -1, j, piece(1) + one, 48 - one)],
        )

    def start_b1(j):
        group(("b1", j), 384, [same("x", step, j, block(0), 192) for step in (1, -1)])

    def start_b2(j):
        group(
            ("b2", j),
            192,
            [same("x", 1, j, block(-1), 96), same("x", -1, j, block(1) + 96, 96)],
        )

    def start_core(j):
        moved["core", j] = links.send("c", 0, wbuf.at[c, j], wbuf.at[c, j])

    over(1, 8, lambda j: row(j).start())
    own.wait()
    start_y1()
    wide = links.send("c", 0, wm, wmb.at[1])
    thin = links.send("c", 0, mup, mup_other)
    start_core(0)
    vall[f] = vimg[...]

    for load in small[1:]:
        load.wait()
    low_img = dot_nt(vimg[...], up[...]).astype(BF16)
    squares_img = jnp.zeros((16, 1), F32)
    for k in range(8):
        loads[k][0].wait()
        rows = jnp.dot(sel, xb[k], preferred_element_type=F32)
        xsel[k] = rows.astype(BF16)
        squares_img = squares_img + jnp.sum(rows * rows, axis=1, keepdims=True)
    inverse_img = lax.rsqrt(squares_img * (1.0 / 8192) + norm_eps)

    all_rows.wait_recv()
    tout[...] = dot_nt(vall[...].reshape(128, 1024), wbuf[c, 0]).astype(BF16).reshape(8, 16, 1024)
    over(1, 8, lambda j: back(j).start())
    timg[f] = tout[f]
    arrived("y1")
    start_y2()
    start_a1(3)
    start_a1(1)

    for k in range(8):
        loads[k][1].wait()
        rsel[k] = jnp.dot(sel, rb[k], preferred_element_type=F32).astype(BF16)
    squares = jnp.zeros((256, 1), F32)
    for k in range(8):
        xs = xb[k].astype(F32)
        squares = squares + jnp.sum(xs * xs, axis=1, keepdims=True)
    inverse = lax.rsqrt(squares * (1.0 / 8192) + norm_eps)

    all_back.wait_recv()
    total_img = jnp.zeros((16, 1), F32)
    for k in range(8):
        grad = timg[k].astype(F32) + adapter_scale * jnp.dot(
            low_img, down_t[:, k * 1024 : (k + 1) * 1024], preferred_element_type=F32
        )
        g = gain[k] * grad
        gained[k] = g
        total_img = total_img + jnp.sum(xsel[k].astype(F32) * g, axis=1, keepdims=True)
    drop_img = inverse_img * inverse_img * inverse_img * (total_img * (1.0 / 8192))
    inside = lax.broadcasted_iota(jnp.int32, (16, 1024), 0) < counts_s[me]
    for k in range(8):
        rows = (
            rsel[k].astype(F32) + inverse_img * gained[k] - xsel[k].astype(F32) * drop_img
        )
        rows = jnp.where(inside, rows, 0.0).astype(BF16)
        for b in range(4):
            visout[k // 2, b, k % 2] = rows[:, b * 256 : (b + 1) * 256]
    over(1, 32, lambda j: spread(j).start())
    vrecv[me] = visout[y, z]
    start_r1()

    p = preact[...].astype(F32)
    normal_cdf = 0.5 * (1.0 + lax.erf(p * 0.7071067811865476))
    act[...] = (p * normal_cdf).astype(BF16)
    slope[...] = normal_cdf + p * (jnp.exp(-0.5 * p * p) * 0.3989422804014327)
    actl[...] = jnp.zeros_like(actl)
    actl[:, 0:16] = dot_nt(act[...], md[...]).astype(BF16)
    alow[me] = actl[...]

    arrived("y2")
    start_a1(2)
    arrived(("a1", 3))
    start_a2(3)
    arrived(("a1", 1))
    start_a2(1)

    low = dot_nt(v[...], up[...]).astype(BF16)
    low_out_ref[:, 0:16] = low
    low_out_ref[:, 16:128] = jnp.zeros((256, 112), BF16)
    low_t = dot_nt(up[...], v[...]).astype(BF16)
    projected_t = jnp.zeros((16, 256), F32)
    for k in range(8):
        normed = (xb[k].astype(F32) * inverse * gain[k]).astype(BF16)
        part1[:, k * 1024 : (k + 1) * 1024] = scale_factor * jnp.dot(
            low_t, normed, preferred_element_type=F32
        )
        projected_t = projected_t + dot_nt(down_t[:, k * 1024 : (k + 1) * 1024], normed)
    sum1 = AdapterSum(links, part1, sums1, bufs1)
    sum1.swap()
    part2[:, 0:1024] = scale_factor * jnp.dot(
        projected_t.astype(BF16), v[...], preferred_element_type=F32
    )
    part2[:, 6144:8192] = jnp.zeros((16, 2048), F32)

    eye = lax.broadcasted_iota(jnp.int32, (32, 32), 0) == lax.broadcasted_iota(
        jnp.int32, (32, 32), 1
    )
    earlier = lax.broadcasted_iota(jnp.int32, (32, 32), 1) < lax.broadcasted_iota(
        jnp.int32, (32, 32), 0
    )
    counts_f = counts[...].astype(F32)
    owners_f = owners[...].astype(F32)
    owner_col = jnp.sum(jnp.where(eye, owners_f, 0.0), axis=1, keepdims=True)
    count_col = jnp.sum(jnp.where(eye, counts_f, 0.0), axis=1, keepdims=True)
    start_col = jnp.sum(
        jnp.where((owner_col == owners_f) & earlier, counts_f, 0.0), axis=1, keepdims=True
    )
    slot = lax.broadcasted_iota(jnp.int32, (32, 512), 1)
    image = lax.broadcasted_iota(jnp.int32, (32, 512), 0)
    inner = (slot % 16).astype(F32)
    key = (
        jnp.sum(
            jnp.where(
                (slot // 16 == image) & (inner < count_col),
                owner_col * 32.0 + start_col + inner + 1.0,
                0.0,
            ),
            axis=0,
            keepdims=True,
        )
        - 1.0
    )

    all_spread.wait_recv()
    wide.wait_recv()
    thin.wait_recv()
    wm_load.wait()
    r = lax.broadcasted_iota(jnp.int32, (512, 1), 0)
    row_id = ((2 * (r // 128) + c) * 4 + (r // 32) % 4) * 32 + r % 32
    pick = jnp.where(row_id.astype(F32) == key, 1.0, 0.0).astype(BF16)
    rows_own[...] = jnp.dot(
        pick, vrecv[:, c].reshape(512, 256), preferred_element_type=F32
    ).astype(BF16)
    rows_other[...] = jnp.dot(
        pick, vrecv[:, 1 - c].reshape(512, 256), preferred_element_type=F32
    ).astype(BF16)
    low_part = dot_nt(rows_own[...], mup[...]) + dot_nt(rows_other[...], mup_other[...])
    lowp[...] = jnp.zeros_like(lowp)
    lowp[:, :, 0:16] = low_part.reshape(16, 32, 16)
    over(1, 16, lambda j: low_row(j).start())
    over(1, 32, lambda j: low_out(j).start())
    sum1.along()
    arrived(("a2", 3))
    start_b1(3)
    arrived(("a1", 2))
    start_a2(2)
    low_hi = low_part.astype(BF16)
    low_lo = (low_part - low_hi.astype(F32)).astype(BF16)

    def columns(n):
        cols = pl.ds(pl.multiple_of(n * 512, 512), 512)
        value = dot_nt(rows_own[...], wmb[0, cols]) + dot_nt(rows_other[...], wmb[1, cols])
        value = value + adapter_scale * (
            jnp.dot(low_hi, md[:, cols], preferred_element_type=F32)
            + jnp.dot(low_lo, md[:, cols], preferred_element_type=F32)
        )
        return value.astype(BF16)

    def fill_a(n):
        value = columns(n)
        cols = pl.ds(pl.multiple_of(n * 512, 512), 512)
        for yy in range(4):
            for zz in range(4):
                at_row = yy * 128 + zz * 32
                qa[zz, yy // 2, (yy % 2) * 32 : (yy % 2) * 32 + 32, cols] = value[
                    at_row : at_row + 32
                ]

    def fill_b(n):
        value = columns(n + 6)
        cols = pl.ds(pl.multiple_of(n * 512, 512), 512)
        qb[:, :, :, cols] = value.reshape(4, 2, 64, 512)

    sum_a = RingSum(links, "z", qa, relay_a, mid_a, near_a)
    sum_b = RingSum(links, "y", qb, relay_b, mid_b, near_b)
    over(0, 6, fill_a)
    sum_a.start()
    arrived(("a2", 1))
    start_b1(1)
    arrived("r1")
    start_r2()
    over(0, 4, fill_b)
    sum_b.start()
    arrived(("a2", 2))
    start_b1(2)

    total = jnp.zeros((256, 1), F32)
    stores = []

    def through_block(cs, j, total):
        k = 2 * lax.rem(y + j, 4) + cs
        value = dot_nt(v[...], wbuf[cs, j]).astype(BF16)
        through[k] = value
        cols = pl.ds(pl.multiple_of(k * 1024, 1024), 1024)
        store = pltpu.make_async_copy(
            through.at[k], through_out.at[:, cols], out_sems.at[len(stores)]
        )
        store.start()
        stores.append(store)
        grad = value.astype(F32) + adapter_scale * jnp.dot(
            low, down_t[:, cols], preferred_element_type=F32
        )
        return total + jnp.sum(xb[k].astype(F32) * (gain[k] * grad), axis=1, keepdims=True)

    all_low_rows.wait_recv()
    lowin[my16] = lowp[my16]
    low_sum = lowin[0]
    for k in range(1, 16):
        low_sum = low_sum + lowin[k]
    low_sum_t = low_sum.T[0:16].astype(BF16)
    part2[:, 1024:6144] = scale_factor * jnp.dot(
        low_sum_t, act[...], preferred_element_type=F32
    )
    sum2 = AdapterSum(links, part2, sums2, bufs2)
    sum2.swap()
    total = through_block(c, 0, total)
    sum2.along()
    arrived(("core", 0))
    total = through_block(1 - c, 0, total)
    sum_a.forward()
    arrived(("b1", 3))
    start_b2(3)
    sum1.across()

    all_low_out.wait_recv()
    every = lax.broadcasted_iota(jnp.int32, (1024, 1), 0).astype(F32)
    pick_all = jnp.where(every == key, 1.0, 0.0).astype(BF16)
    low_slots = dot_tn(alow[...].reshape(1024, 128), pick_all).astype(BF16)
    mpart[...] = scale_factor * jnp.dot(
        low_slots[0:16], vrecv[:, c].reshape(512, 256), preferred_element_type=F32
    )
    msum = links.group([("x", k, mpart, mr.at[k - 1]) for k in (1, 2, 3)], mr)
    sum_b.forward()
    arrived(("b1", 1))
    start_b2(1)
    def into(ref):
        def put(half, span, value):
            i = span.start // 16
            ref[2 * half + i // 2, lax.rem(i, 2)] = value.astype(BF16)

        return put

    sum_a.finish(into(next_a))
    sum_c = RingSum(links, "y", next_a, relay_c, mid_c, near_c)
    sum_c.start()
    arrived(("b1", 2))
    start_b2(2)
    sum1.back()
    sum_b.finish(into(next_b))
    sum_d = RingSum(links, "z", next_b, relay_d, mid_d, near_d)
    sum_d.start()
    sum2.across()
    arrived("r2")
    arrived(("b2", 3))
    start_core(3)
    total = through_block(c, 3, total)
    arrived(("b2", 1))
    start_core(1)
    total = through_block(c, 1, total)
    sum1.outward()
    sum2.back()
    sum_c.forward()
    sum_d.forward()
    arrived(("core", 3))
    total = through_block(1 - c, 3, total)
    arrived(("b2", 2))
    start_core(2)
    total = through_block(c, 2, total)
    sum2.outward()
    sum1.last()
    arrived(("core", 1))
    total = through_block(1 - c, 1, total)

    def result(at):
        def put(half, span, value):
            cols = slice(at, at + value.shape[1])
            rows = slice(half * 16, half * 16 + 16)
            pgrad[rows, cols] = (value * slope[rows, cols]).astype(BF16)

        return put

    sum_c.finish(result(0))
    sum_d.finish(result(next_a.shape[-1]))
    msum.wait_recv()
    mout[...] = (mpart[...] + mr[0]) + (mr[1] + mr[2])
    sum2.last()
    arrived(("core", 2))
    total = through_block(1 - c, 2, total)
    sum1.end()
    sum2.end()
    inverse_out[...] = jnp.broadcast_to(inverse, (256, 128))
    drop = inverse * inverse * inverse * (total * (1.0 / 8192))
    drop_out[...] = jnp.broadcast_to(drop, (256, 128))

    for store in stores:
        store.wait()
    for copies in (all_rows, all_back, all_spread, all_low_out, all_low_rows):
        copies.wait_send()
    links.finish()


def big_call(scale_factor, *args):
    dma = pltpu.SemaphoreType.DMA
    wide_a, wide_b = 3072, 2048

    def big(w):
        return [
            pltpu.VMEM((2, 64, w), BF16),
            pltpu.VMEM((2, 64, w), BF16),
            pltpu.VMEM((2, 2, 64, w), BF16),
            pltpu.VMEM((4, 2, 16, w), BF16),
        ]

    def small(w):
        return [
            pltpu.VMEM((2, 16, w), BF16),
            pltpu.VMEM((2, 16, w), BF16),
            pltpu.VMEM((2, 2, 16, w), BF16),
        ]

    def sums():
        return [
            pltpu.VMEM((8, 8192), F32),
            pltpu.VMEM((4, 8, 2048), F32),
            pltpu.VMEM((3, 8, 2048), F32),
            pltpu.VMEM((16, 8, 128), F32),
            pltpu.VMEM((16, 8, 128), F32),
            pltpu.VMEM((4, 16, 8, 128), F32),
            pltpu.VMEM((4, 16, 8, 128), F32),
        ]

    scalar = pl.BlockSpec(memory_space=pltpu.SMEM)
    shape = jax.ShapeDtypeStruct
    return pl.pallas_call(
        functools.partial(big_kernel, scale_factor),
        out_shape=(
            shape((256, 8192), BF16),
            shape((256, 128), BF16),
            shape((256, 128), F32),
            shape((256, 128), F32),
            shape((32, 5120), BF16),
            shape((16, 8192), F32),
            shape((16, 8192), F32),
            shape((16, 256), F32),
        ),
        in_specs=[scalar, scalar] + [VMEM] * 4 + [ANY] * 9,
        out_specs=(ANY,) + (VMEM,) * 7,
        scratch_shapes=[
            pltpu.VMEM((2, 4, 1024, 1024), BF16),
            pltpu.VMEM((8, 256, 1024), BF16),
            pltpu.VMEM((8, 256, 1024), BF16),
            pltpu.VMEM((8, 256, 1024), BF16),
            dma((64,)), dma((64,)), dma((23,)), dma((8,)),
            pltpu.VMEM((256, 1024), BF16),
            pltpu.VMEM((8, 1, 1024), F32),
            pltpu.VMEM((16, 8192), BF16),
            pltpu.VMEM((32, 5120), BF16),
            pltpu.VMEM((16, 5120), BF16),
            pltpu.VMEM((32, 5120), F32),
            pltpu.VMEM((16, 1024), BF16),
            pltpu.VMEM((8, 16, 1024), BF16),
            pltpu.VMEM((8, 16, 1024), BF16),
            pltpu.VMEM((8, 16, 1024), BF16),
            pltpu.VMEM((8, 16, 1024), BF16),
            pltpu.VMEM((8, 16, 1024), BF16),
            pltpu.VMEM((8, 16, 1024), F32),
            pltpu.VMEM((4, 4, 2, 16, 256), BF16),
            pltpu.VMEM((32, 2, 16, 256), BF16),
            pltpu.VMEM((32, 128), BF16),
            pltpu.VMEM((32, 32, 128), BF16),
            pltpu.VMEM((32, 5120), BF16),
            pltpu.VMEM((2, 5120, 256), BF16),
            pltpu.VMEM((16, 256), BF16),
            pltpu.VMEM((16, 32, 128), F32),
            pltpu.VMEM((16, 32, 128), F32),
            pltpu.VMEM((512, 256), BF16),
            pltpu.VMEM((512, 256), BF16),
            pltpu.VMEM((16, 256), F32),
            pltpu.VMEM((3, 16, 256), F32),
            pltpu.VMEM((4, 2, 64, wide_a), BF16),
            pltpu.VMEM((4, 2, 64, wide_b), BF16),
            *big(wide_a), *big(wide_b), *small(wide_a), *small(wide_b),
            pltpu.VMEM((16, 8192), F32),
            pltpu.VMEM((16, 8192), F32),
            *sums(), *sums(),
        ],
        compiler_params=pltpu.CompilerParams(
            collective_id=0, has_side_effects=True, vmem_limit_bytes=67_043_328
        ),
        name="big",
    )(*args)


def finish_kernel(
    mup, hidden, resid, through, sums1, sums2,
    gain_in, down_in, low_in, inverse_in, drop_in, pgrad_in,
    out, pgrad_out, vdown, vup, mdown, mup_out,
    hb, rb, tb, one, two, gain, down_t, low, inverse, drop, pgrad,
    load_sems, out_sems, sum_sems, small_sems,
):
    small = []
    pairs = (
        (gain_in, gain), (down_in, down_t), (low_in, low), (inverse_in, inverse),
        (drop_in, drop), (pgrad_in, pgrad),
    )
    for n, (src, dst) in enumerate(pairs):
        small.append(pltpu.make_async_copy(src, dst, small_sems.at[n]))
        small[n].start()
    loads = []

    def load(k):
        cols = pl.ds(k * 1024, 1024)
        loads.append(
            [
                pltpu.make_async_copy(src.at[:, cols], dst.at[k], load_sems.at[n, k])
                for n, (src, dst) in enumerate(((through, tb), (hidden, hb), (resid, rb)))
            ]
        )
        for copy in loads[k]:
            copy.start()

    for k in range(3):
        load(k)
    sums_in = [
        pltpu.make_async_copy(sums1, one, sum_sems.at[0]),
        pltpu.make_async_copy(sums2, two, sum_sems.at[1]),
    ]
    for copy in small:
        copy.wait()
    mup_out[...] = mup[...]
    stores = []
    for k in range(8):
        cols = slice(k * 1024, (k + 1) * 1024)
        for copy in loads[k]:
            copy.wait()
        if k < 5:
            load(k + 3)
        if k == 4:
            for copy in sums_in:
                copy.start()
        grad = tb[k].astype(F32) + adapter_scale * jnp.dot(
            low[:, 0:16], down_t[:, cols], preferred_element_type=F32
        )
        rows = (
            rb[k].astype(F32)
            + inverse[:, 0:1] * (gain[k] * grad)
            - hb[k].astype(F32) * drop[:, 0:1]
        )
        tb[k] = rows.astype(BF16)
        store = pltpu.make_async_copy(tb.at[k], out.at[:, pl.ds(k * 1024, 1024)], out_sems.at[k])
        store.start()
        stores.append(store)
    for copy in sums_in:
        copy.wait()
    stores += [
        pltpu.make_async_copy(pgrad, pgrad_out, small_sems.at[6]),
        pltpu.make_async_copy(one, vdown, sum_sems.at[2]),
        pltpu.make_async_copy(two.at[:, pl.ds(0, 1024)], vup, sum_sems.at[3]),
        pltpu.make_async_copy(two.at[:, pl.ds(1024, 5120)], mdown, sum_sems.at[4]),
    ]
    for store in stores[8:]:
        store.start()
    for store in stores:
        store.wait()


def finish(*args):
    dma = pltpu.SemaphoreType.DMA
    shape = jax.ShapeDtypeStruct
    return pl.pallas_call(
        finish_kernel,
        out_shape=(
            shape((256, 8192), BF16),
            shape((32, 5120), BF16),
            shape((16, 8192), F32),
            shape((16, 1024), F32),
            shape((16, 5120), F32),
            shape((16, 256), F32),
        ),
        in_specs=[VMEM] + [ANY] * 11,
        out_specs=(ANY, ANY, ANY, ANY, ANY, VMEM),
        scratch_shapes=[
            pltpu.VMEM((8, 256, 1024), BF16),
            pltpu.VMEM((8, 256, 1024), BF16),
            pltpu.VMEM((8, 256, 1024), BF16),
            pltpu.VMEM((16, 8192), F32),
            pltpu.VMEM((16, 8192), F32),
            pltpu.VMEM((8, 1, 1024), F32),
            pltpu.VMEM((16, 8192), BF16),
            pltpu.VMEM((256, 128), BF16),
            pltpu.VMEM((256, 128), F32),
            pltpu.VMEM((256, 128), F32),
            pltpu.VMEM((32, 5120), BF16),
            dma((3, 8)), dma((8,)), dma((5,)), dma((7,)),
        ],
        compiler_params=pltpu.CompilerParams(vmem_limit_bytes=67_043_328),
        name="finish",
    )(*args)


def body(
    hidden,
    residual_gradient,
    value_output_gradient,
    attention_norm_gain,
    value_frozen_weight,
    value_down_factor,
    value_up_factor,
    merger_frozen_weight,
    merger_down_factor,
    merger_up_factor,
    merger_saved_preactivation,
    image_token_counts,
    image_encoder_owner,
    image_first_rows,
):
    scale_factor = 256.0 / (hidden.shape[0] * 128) * adapter_scale
    gain = attention_norm_gain.reshape(8, 1, 1024)
    down_t = value_down_factor.T
    through, low, inverse, drop, pgrad, sums1, sums2, mup_sum = big_call(
        scale_factor,
        image_first_rows,
        image_token_counts,
        image_token_counts.reshape(1, 32),
        image_encoder_owner.reshape(1, 32),
        value_up_factor,
        merger_up_factor,
        value_output_gradient,
        gain,
        down_t,
        merger_saved_preactivation,
        merger_down_factor.T,
        hidden,
        residual_gradient,
        value_frozen_weight,
        merger_frozen_weight,
    )
    layer_input_gradient, preactivation_gradient, vdown, vup, mdown, merger_up_gradient = finish(
        mup_sum,
        hidden,
        residual_gradient,
        through,
        sums1,
        sums2,
        gain,
        down_t,
        low,
        inverse,
        drop,
        pgrad,
    )
    return (
        layer_input_gradient,
        preactivation_gradient,
        vdown.T,
        vup,
        mdown.T,
        merger_up_gradient,
    )


def solution(mesh):
    tokens = P(("dp", "fsdp", "enc"), None)
    features = P(None, ("fsdp", "enc"))
    placed = (
        tokens,
        tokens,
        tokens,
        P(),
        P("fsdp", None),
        P(),
        P(),
        features,
        P(),
        features,
        tokens,
        P("dp"),
        P("dp"),
        P(("dp", "fsdp", "enc")),
    )
    return jax.shard_map(
        body,
        mesh=mesh,
        in_specs=placed,
        out_specs=(tokens, tokens, P(), P(), P(), features),
        check_vma=False,
    )
```

```python
import functools

import jax
import jax.numpy as jnp
from jax import lax
from jax.experimental import pallas as pl
from jax.experimental.pallas import tpu as pltpu
from jax.sharding import PartitionSpec as P

MAXIMG = 16
adapter_scale = 2.0
norm_eps = 1e-06
F32, BF16 = jnp.float32, jnp.bfloat16
MESH = pl.DeviceIdType.MESH
VMEM = pl.BlockSpec(memory_space=pltpu.VMEM)
ANY = pl.BlockSpec(memory_space=pl.ANY)


def dot_nt(a, b):
    return lax.dot_general(a, b, (((1,), (1,)), ((), ())), preferred_element_type=F32)


def dot_tn(a, b):
    return lax.dot_general(a, b, (((0,), (0,)), ((), ())), preferred_element_type=F32)


def wrap(v, n):
    return lax.rem(v + n, n)


def place():
    f = lax.axis_index("fsdp")
    return lax.axis_index("dp"), f // 2, lax.axis_index("enc"), lax.rem(f, 2)


class Links:
    def __init__(self, send_sems, recv_sems):
        self.x, self.y, self.z, self.c = place()
        self.send_sems, self.recv_sems = send_sems, recv_sems
        self.made = []
        self.taken = 0

    def peer(self, axis, step):
        if axis == "x":
            return {"dp": wrap(self.x + step, 4)}
        if axis == "z":
            return {"enc": wrap(self.z + step, 4)}
        if axis == "y":
            return {"fsdp": 2 * wrap(self.y + step, 4) + self.c}
        return {"fsdp": 2 * self.y + 1 - self.c}

    def take(self):
        self.taken += 1
        return self.send_sems.at[self.taken - 1], self.recv_sems.at[self.taken - 1]

    def send(self, axis, step, src, dst):
        return self.group([(axis, step, src, dst)], dst)

    def group(self, sends, whole):
        sems = self.take()
        for axis, step, src, dst in sends:
            self.copy(sems, src, dst, self.peer(axis, step)).start()
        total = self.copy(sems, whole, whole, self.peer(*sends[0][:2]))
        self.made.append(total)
        return total

    def copy(self, sems, src, dst, peer):
        return pltpu.make_async_remote_copy(
            src_ref=src,
            dst_ref=dst,
            send_sem=sems[0],
            recv_sem=sems[1],
            device_id=peer,
            device_id_type=MESH,
        )

    def finish(self):
        for copy in self.made:
            copy.wait_send()

    def meet(self, peers):
        barrier = pltpu.get_barrier_semaphore()
        for axis, step in peers:
            pl.semaphore_signal(barrier, inc=1, device_id=self.peer(axis, step), device_id_type=MESH)
        pl.semaphore_wait(barrier, len(peers))


def chunked(count, act):
    def step(i, carry):
        act(pl.ds(pl.multiple_of(i * 16, 16), 16))
        return carry

    lax.fori_loop(0, count // 16, step, 0)


class RingSum:
    def __init__(self, links, axis, blocks, relay, mid, near):
        self.links, self.axis, self.blocks = links, axis, blocks
        self.relay, self.mid, self.near = relay, mid, near
        m = links.x if axis == "x" else links.y if axis == "y" else links.z
        self.me, self.count = m, blocks.shape[2]

    def start(self):
        send, b, axis = self.links.send, self.blocks, self.axis
        far = wrap(self.me + 2, 4)
        right, left = wrap(self.me + 1, 4), wrap(self.me - 1, 4)
        self.far = [
            send(axis, 1, b.at[far, 0], self.relay.at[0]),
            send(axis, -1, b.at[far, 1], self.relay.at[1]),
        ]
        self.direct = [
            send(axis, 1, b.at[right, 1], self.near.at[0, 1]),
            send(axis, -1, b.at[left, 0], self.near.at[1, 0]),
        ]

    def forward(self):
        for way, step in ((0, 1), (1, -1)):
            self.far[way].wait_recv()
            to = wrap(self.me + step, 4)

            def add(span, way=way, to=to):
                self.mid[way, span] = (
                    self.blocks[to, way, span].astype(F32) + self.relay[way, span].astype(F32)
                ).astype(BF16)

            chunked(self.count, add)
            self.direct.append(
                self.links.send(self.axis, step, self.mid.at[way], self.near.at[way, way])
            )

    def finish(self, put):
        for copy in self.direct:
            copy.wait_recv()
        for half in range(2):

            def add(span, half=half):
                put(
                    half,
                    span,
                    self.blocks[self.me, half, span].astype(F32)
                    + self.near[0, half, span].astype(F32)
                    + self.near[1, half, span].astype(F32),
                )

            chunked(self.count, add)


class AdapterSum:
    def __init__(self, links, src, out, bufs):
        self.links, self.src, self.out = links, src, out
        self.half_in, self.ay, self.ry, self.bxz, self.rxz, self.gy, self.gc = bufs
        self.sems = links.take(), links.take()
        self.m16 = links.x * 4 + links.z
        self.other = pl.ds(pl.multiple_of((1 - links.c) * 8, 8), 8)
        self.mine = pl.ds(pl.multiple_of(links.c * 8, 8), 8)

    def plane(self, k):
        d = lax.rem(self.m16 + k, 16)
        return {"dp": d // 4, "enc": lax.rem(d, 4)}

    def spread(self, k):
        return self.links.copy(
            self.sems[0], self.bxz.at[lax.rem(self.m16 + k, 16)], self.rxz.at[k - 1], self.plane(k)
        )

    def share(self, k):
        here = self.gy.at[self.links.y, self.m16]
        return self.links.copy(self.sems[1], here, here, self.plane(k))

    def total(self, n):
        whole = self.rxz.at[0:15]
        return self.links.copy(self.sems[n], whole, whole, self.plane(1))

    def swap(self):
        self.swapped = self.links.send("c", 0, self.src.at[self.other], self.half_in)

    def along(self):
        self.swapped.wait_recv()
        for b in range(4):
            cols = slice(b * 2048, (b + 1) * 2048)
            self.ay[b] = self.src[self.mine, cols] + self.half_in[:, cols]
        y = self.links.y
        self.sent = self.links.group(
            [("y", k, self.ay.at[wrap(y + k, 4)], self.ry.at[k - 1]) for k in (1, 2, 3)], self.ry
        )

    def across(self):
        self.sent.wait_recv()
        here = self.ay.at[self.links.y]
        for b in range(16):
            cols = slice(b * 128, (b + 1) * 128)
            self.bxz[b] = (here[:, cols] + self.ry[0, :, cols]) + (
                self.ry[1, :, cols] + self.ry[2, :, cols]
            )
        over(1, 16, lambda k: self.spread(k).start())

    def back(self):
        self.total(0).wait_recv()
        value = self.bxz[self.m16]
        for k in range(15):
            value = value + self.rxz[k]
        self.gy[self.links.y, self.m16] = value
        over(1, 16, lambda k: self.share(k).start())

    def outward(self):
        self.total(1).wait_recv()
        here = self.gy.at[self.links.y]
        self.wide = self.links.group(
            [("y", k, here, here) for k in (1, 2, 3)], self.gy.at[0:3]
        )

    def last(self):
        self.wide.wait_recv()
        self.final = self.links.send("c", 0, self.gy, self.gc)
        for b in range(64):
            self.out[self.mine, b * 128 : (b + 1) * 128] = self.gy[b // 16, b % 16]

    def end(self):
        self.final.wait_recv()
        for b in range(64):
            self.out[self.other, b * 128 : (b + 1) * 128] = self.gc[b // 16, b % 16]
        self.total(0).wait_send()
        self.total(1).wait_send()


def over(lo, hi, act):
    def step(j, carry):
        act(j)
        return carry

    lax.fori_loop(lo, hi, step, 0)


def big_kernel(
    scale_factor,
    first_row, counts_s, counts, owners, up, mup,
    v_in, gain_in, down_in, preact_in, md_in, hidden, resid, wsh, wm,
    through_out, low_out_ref, inverse_out, drop_out, pgrad, sums1, sums2, mout,
    wbuf, xb, rb, through, send_sems, recv_sems, local_sems, out_sems,
    v, gain, down_t, preact, md, slope,
    vimg, xsel, rsel, vall, tout, timg, gained, visout, vrecv, actl, alow, act,
    wmb, mup_other, lowp, lowin, rows_own, rows_other, mpart, mr,
    qa, qb,
    relay_a, mid_a, near_a, next_a, relay_b, mid_b, near_b, next_b,
    relay_c, mid_c, near_c, relay_d, mid_d, near_d,
    part1, part2, *rest,
):
    bufs1, bufs2 = rest[:7], rest[7:14]
    links = Links(send_sems, recv_sems)
    x, y, z, c = links.x, links.y, links.z, links.c
    f = 2 * y + c
    me = f * 4 + z

    small = []
    pairs = ((v_in, v), (gain_in, gain), (down_in, down_t), (preact_in, preact), (md_in, md))
    for n, (src, dst) in enumerate(pairs):
        small.append(pltpu.make_async_copy(src, dst, local_sems.at[18 + n]))
        small[n].start()
    own = pltpu.make_async_copy(wsh, wbuf.at[c, 0], local_sems.at[0])
    own.start()
    loads = []
    for k in range(8):
        cols = pl.ds(k * 1024, 1024)
        a = pltpu.make_async_copy(hidden.at[:, cols], xb.at[k], local_sems.at[1 + k])
        b = pltpu.make_async_copy(resid.at[:, cols], rb.at[k], local_sems.at[9 + k])
        a.start()
        b.start()
        loads.append((a, b))
    wm_load = pltpu.make_async_copy(wm, wmb.at[0], local_sems.at[17])
    wm_load.start()

    barrier = pltpu.get_barrier_semaphore()

    def plane_peer(j):
        d = lax.rem(me + j, 32)
        return {"fsdp": d // 4, "enc": lax.rem(d, 4)}

    def greet(j):
        pl.semaphore_signal(barrier, inc=1, device_id=plane_peer(j), device_id_type=MESH)

    def greet_x(j):
        d = 4 + j
        pl.semaphore_signal(
            barrier,
            inc=1,
            device_id={"dp": lax.rem(x + d // 4, 4), "enc": lax.rem(z + d, 4)},
            device_id_type=MESH,
        )

    over(1, 32, greet)
    over(0, 12, greet_x)
    first = first_row[0]
    lane = lax.broadcasted_iota(jnp.int32, (16, 256), 1)
    line = lax.broadcasted_iota(jnp.int32, (16, 256), 0)
    sel = jnp.where(lane == line + first, 1.0, 0.0).astype(BF16)
    small[0].wait()
    vimg[...] = jnp.dot(sel, v[...], preferred_element_type=F32).astype(BF16)
    pl.semaphore_wait(barrier, 43)

    sems_row, sems_back, sems_spread = links.take(), links.take(), links.take()
    sems_low_out, sems_low_row = links.take(), links.take()
    my16 = y * 4 + z

    def row(j):
        return links.copy(sems_row, vimg, vall.at[f], {"fsdp": lax.rem(f + j, 8)})

    def back(j):
        to = lax.rem(f + j, 8)
        return links.copy(sems_back, tout.at[to], timg.at[f], {"fsdp": to})

    def spread(j):
        d = lax.rem(me + j, 32)
        return links.copy(sems_spread, visout.at[d // 8, lax.rem(d, 4)], vrecv.at[me], plane_peer(j))

    def low_out(j):
        return links.copy(sems_low_out, actl, alow.at[me], plane_peer(j))

    def low_row(j):
        d = lax.rem(my16 + j, 16)
        peer = {"fsdp": 2 * (d // 4) + c, "enc": lax.rem(d, 4)}
        return links.copy(sems_low_row, lowp.at[d], lowin.at[my16], peer)

    def all_of(sems, whole):
        return links.copy(sems, whole, whole, plane_peer(1))

    all_rows = all_of(sems_row, vall.at[0:7])
    all_back = all_of(sems_back, timg.at[0:7])
    all_spread = all_of(sems_spread, vrecv.at[0:31])
    all_low_out = all_of(sems_low_out, alow.at[0:31])
    all_low_rows = all_of(sems_low_row, lowin.at[0:15])

    def at(j, start, count):
        return wbuf.at[c, j, pl.ds(pl.multiple_of(start, 16), count)]

    def piece(step):
        return (x * 4 + wrap(z + step, 4)) * 48

    def block(step):
        return wrap(x + step, 4) * 192

    def early(step):
        return 768 + wrap(x + step, 4) * 64

    moved = {}

    def arrived(name):
        moved[name].wait_recv()

    def group(name, rows, sends):
        moved[name] = links.group(sends, wbuf.at[c, 0, 0:rows])

    def start_y1():
        src = at(0, piece(0), 48)
        group("y1", 96, [("y", t, src, at(j, piece(0), 48)) for t, j in ((1, 3), (-1, 1))])

    def start_y2():
        sends = []
        for t, j, start, count in ((1, 3, piece(0), 32), (-1, 1, piece(0) + 32, 16)):
            sends.append(("y", t, at(j, start, count), at(2, start, count)))
        group("y2", 48, sends)

    def start_r1():
        src = at(0, early(0), 64)
        group("r1", 128, [("y", t, src, at(j, early(0), 64)) for t, j in ((1, 3), (-1, 1))])

    def start_r2():
        sends = []
        for t, j, start in ((1, 3, early(0)), (-1, 1, early(0) + 32)):
            sends.append(("y", t, at(j, start, 32), at(2, start, 32)))
        group("r2", 64, sends)

    def start_c1(j):
        group(("c1", j), 128, [same("x", step, j, early(0), 64) for step in (1, -1)])

    def start_c2(j):
        group(
            ("c2", j),
            64,
            [same("x", 1, j, early(-1), 32), same("x", -1, j, early(1) + 32, 32)],
        )

    def same(axis, step, j, start, count):
        here = at(j, start, count)
        return (axis, step, here, here)

    def start_a1(j):
        group(("a1", j), 96, [same("z", step, j, piece(0), 48) for step in (1, -1)])

    def start_a2(j):
        one = 32 if j == 3 else 16
        group(
            ("a2", j),
            48,
            [same("z", 1, j, piece(-1), one), same("z", -1, j, piece(1) + one, 48 - one)],
        )

    def start_b1(j):
        group(("b1", j), 384, [same("x", step, j, block(0), 192) for step in (1, -1)])

    def start_b2(j):
        group(
            ("b2", j),
            192,
            [same("x", 1, j, block(-1), 96), same("x", -1, j, block(1) + 96, 96)],
        )

    def start_core(j):
        if j:
            arrived(("c2", j))
        moved["core", j] = links.send("c", 0, wbuf.at[c, j], wbuf.at[c, j])

    over(1, 8, lambda j: row(j).start())
    own.wait()
    start_y1()
    start_r1()
    wide = links.send("c", 0, wm, wmb.at[1])
    thin = links.send("c", 0, mup, mup_other)
    start_core(0)
    vall[f] = vimg[...]

    for load in small[1:]:
        load.wait()
    low_img = dot_nt(vimg[...], up[...]).astype(BF16)
    squares_img = jnp.zeros((16, 1), F32)
    for k in range(8):
        loads[k][0].wait()
        rows = jnp.dot(sel, xb[k], preferred_element_type=F32)
        xsel[k] = rows.astype(BF16)
        squares_img = squares_img + jnp.sum(rows * rows, axis=1, keepdims=True)
    inverse_img = lax.rsqrt(squares_img * (1.0 / 8192) + norm_eps)

    all_rows.wait_recv()
    tout[...] = dot_nt(vall[...].reshape(128, 1024), wbuf[c, 0]).astype(BF16).reshape(8, 16, 1024)
    over(1, 8, lambda j: back(j).start())
    timg[f] = tout[f]
    arrived("y1")
    start_y2()
    start_a1(3)
    start_a1(1)
    arrived("r1")
    start_r2()
    start_c1(3)
    start_c1(1)

    for k in range(8):
        loads[k][1].wait()
        rsel[k] = jnp.dot(sel, rb[k], preferred_element_type=F32).astype(BF16)
    squares = jnp.zeros((256, 1), F32)
    for k in range(8):
        xs = xb[k].astype(F32)
        squares = squares + jnp.sum(xs * xs, axis=1, keepdims=True)
    inverse = lax.rsqrt(squares * (1.0 / 8192) + norm_eps)

    all_back.wait_recv()
    total_img = jnp.zeros((16, 1), F32)
    for k in range(8):
        grad = timg[k].astype(F32) + adapter_scale * jnp.dot(
            low_img, down_t[:, k * 1024 : (k + 1) * 1024], preferred_element_type=F32
        )
        g = gain[k] * grad
        gained[k] = g
        total_img = total_img + jnp.sum(xsel[k].astype(F32) * g, axis=1, keepdims=True)
    drop_img = inverse_img * inverse_img * inverse_img * (total_img * (1.0 / 8192))
    inside = lax.broadcasted_iota(jnp.int32, (16, 1024), 0) < counts_s[me]
    for k in range(8):
        rows = (
            rsel[k].astype(F32) + inverse_img * gained[k] - xsel[k].astype(F32) * drop_img
        )
        rows = jnp.where(inside, rows, 0.0).astype(BF16)
        for b in range(4):
            visout[k // 2, b, k % 2] = rows[:, b * 256 : (b + 1) * 256]
    over(1, 32, lambda j: spread(j).start())
    vrecv[me] = visout[y, z]

    p = preact[...].astype(F32)
    normal_cdf = 0.5 * (1.0 + lax.erf(p * 0.7071067811865476))
    act[...] = (p * normal_cdf).astype(BF16)
    slope[...] = normal_cdf + p * (jnp.exp(-0.5 * p * p) * 0.3989422804014327)
    actl[...] = jnp.zeros_like(actl)
    actl[:, 0:16] = dot_nt(act[...], md[...]).astype(BF16)
    alow[me] = actl[...]

    arrived("y2")
    start_a1(2)
    arrived("r2")
    start_c1(2)
    arrived(("c1", 3))
    start_c2(3)
    arrived(("c1", 1))
    start_c2(1)
    arrived(("a1", 3))
    start_a2(3)
    arrived(("a1", 1))
    start_a2(1)

    low = dot_nt(v[...], up[...]).astype(BF16)
    low_out_ref[:, 0:16] = low
    low_out_ref[:, 16:128] = jnp.zeros((256, 112), BF16)
    low_t = dot_nt(up[...], v[...]).astype(BF16)
    projected_t = jnp.zeros((16, 256), F32)
    for k in range(8):
        normed = (xb[k].astype(F32) * inverse * gain[k]).astype(BF16)
        part1[:, k * 1024 : (k + 1) * 1024] = scale_factor * jnp.dot(
            low_t, normed, preferred_element_type=F32
        )
        projected_t = projected_t + dot_nt(down_t[:, k * 1024 : (k + 1) * 1024], normed)
    sum1 = AdapterSum(links, part1, sums1, bufs1)
    sum1.swap()
    part2[:, 0:1024] = scale_factor * jnp.dot(
        projected_t.astype(BF16), v[...], preferred_element_type=F32
    )
    part2[:, 6144:8192] = jnp.zeros((16, 2048), F32)

    eye = lax.broadcasted_iota(jnp.int32, (32, 32), 0) == lax.broadcasted_iota(
        jnp.int32, (32, 32), 1
    )
    earlier = lax.broadcasted_iota(jnp.int32, (32, 32), 1) < lax.broadcasted_iota(
        jnp.int32, (32, 32), 0
    )
    counts_f = counts[...].astype(F32)
    owners_f = owners[...].astype(F32)
    owner_col = jnp.sum(jnp.where(eye, owners_f, 0.0), axis=1, keepdims=True)
    count_col = jnp.sum(jnp.where(eye, counts_f, 0.0), axis=1, keepdims=True)
    start_col = jnp.sum(
        jnp.where((owner_col == owners_f) & earlier, counts_f, 0.0), axis=1, keepdims=True
    )
    slot = lax.broadcasted_iota(jnp.int32, (32, 512), 1)
    image = lax.broadcasted_iota(jnp.int32, (32, 512), 0)
    inner = (slot % 16).astype(F32)
    key = (
        jnp.sum(
            jnp.where(
                (slot // 16 == image) & (inner < count_col),
                owner_col * 32.0 + start_col + inner + 1.0,
                0.0,
            ),
            axis=0,
            keepdims=True,
        )
        - 1.0
    )

    all_spread.wait_recv()
    wide.wait_recv()
    thin.wait_recv()
    wm_load.wait()
    r = lax.broadcasted_iota(jnp.int32, (512, 1), 0)
    row_id = ((2 * (r // 128) + c) * 4 + (r // 32) % 4) * 32 + r % 32
    pick = jnp.where(row_id.astype(F32) == key, 1.0, 0.0).astype(BF16)
    rows_own[...] = jnp.dot(
        pick, vrecv[:, c].reshape(512, 256), preferred_element_type=F32
    ).astype(BF16)
    rows_other[...] = jnp.dot(
        pick, vrecv[:, 1 - c].reshape(512, 256), preferred_element_type=F32
    ).astype(BF16)
    low_part = dot_nt(rows_own[...], mup[...]) + dot_nt(rows_other[...], mup_other[...])
    lowp[...] = jnp.zeros_like(lowp)
    lowp[:, :, 0:16] = low_part.reshape(16, 32, 16)
    over(1, 16, lambda j: low_row(j).start())
    over(1, 32, lambda j: low_out(j).start())
    sum1.along()
    arrived(("a2", 3))
    start_b1(3)
    arrived(("a1", 2))
    start_a2(2)
    arrived(("c1", 2))
    start_c2(2)
    low_hi = low_part.astype(BF16)
    low_lo = (low_part - low_hi.astype(F32)).astype(BF16)

    def columns(n):
        cols = pl.ds(pl.multiple_of(n * 512, 512), 512)
        value = dot_nt(rows_own[...], wmb[0, cols]) + dot_nt(rows_other[...], wmb[1, cols])
        value = value + adapter_scale * (
            jnp.dot(low_hi, md[:, cols], preferred_element_type=F32)
            + jnp.dot(low_lo, md[:, cols], preferred_element_type=F32)
        )
        return value.astype(BF16)

    def fill_a(n):
        value = columns(n)
        cols = pl.ds(pl.multiple_of(n * 512, 512), 512)
        for yy in range(4):
            for zz in range(4):
                at_row = yy * 128 + zz * 32
                qa[zz, yy // 2, (yy % 2) * 32 : (yy % 2) * 32 + 32, cols] = value[
                    at_row : at_row + 32
                ]

    def fill_b(n):
        value = columns(n + 5)
        cols = pl.ds(pl.multiple_of(n * 512, 512), 512)
        qb[:, :, :, cols] = value.reshape(4, 2, 64, 512)

    sum_a = RingSum(links, "z", qa, relay_a, mid_a, near_a)
    sum_b = RingSum(links, "y", qb, relay_b, mid_b, near_b)
    over(0, 5, fill_a)
    sum_a.start()
    arrived(("a2", 1))
    start_b1(1)
    over(0, 5, fill_b)
    sum_b.start()
    sum1.across()
    arrived(("a2", 2))
    start_b1(2)

    total = jnp.zeros((256, 1), F32)
    stores = []

    def through_block(cs, j, total):
        k = 2 * lax.rem(y + j, 4) + cs
        value = dot_nt(v[...], wbuf[cs, j]).astype(BF16)
        through[k] = value
        cols = pl.ds(pl.multiple_of(k * 1024, 1024), 1024)
        store = pltpu.make_async_copy(
            through.at[k], through_out.at[:, cols], out_sems.at[len(stores)]
        )
        store.start()
        stores.append(store)
        grad = value.astype(F32) + adapter_scale * jnp.dot(
            low, down_t[:, cols], preferred_element_type=F32
        )
        return total + jnp.sum(xb[k].astype(F32) * (gain[k] * grad), axis=1, keepdims=True)

    all_low_rows.wait_recv()
    lowin[my16] = lowp[my16]
    low_sum = lowin[0]
    for k in range(1, 16):
        low_sum = low_sum + lowin[k]
    low_sum_t = low_sum.T[0:16].astype(BF16)
    part2[:, 1024:6144] = scale_factor * jnp.dot(
        low_sum_t, act[...], preferred_element_type=F32
    )
    sum2 = AdapterSum(links, part2, sums2, bufs2)
    sum2.swap()
    total = through_block(c, 0, total)
    sum2.along()
    arrived(("core", 0))
    total = through_block(1 - c, 0, total)
    sum_a.forward()
    arrived(("b1", 3))
    start_b2(3)

    all_low_out.wait_recv()
    every = lax.broadcasted_iota(jnp.int32, (1024, 1), 0).astype(F32)
    pick_all = jnp.where(every == key, 1.0, 0.0).astype(BF16)
    low_slots = dot_tn(alow[...].reshape(1024, 128), pick_all).astype(BF16)
    mpart[...] = scale_factor * jnp.dot(
        low_slots[0:16], vrecv[:, c].reshape(512, 256), preferred_element_type=F32
    )
    msum = links.group([("x", k, mpart, mr.at[k - 1]) for k in (1, 2, 3)], mr)
    sum_b.forward()
    arrived(("b1", 1))
    start_b2(1)
    def into(ref):
        def put(half, span, value):
            i = span.start // 16
            ref[2 * half + i // 2, lax.rem(i, 2)] = value.astype(BF16)

        return put

    sum1.back()
    sum_a.finish(into(next_a))
    sum_c = RingSum(links, "y", next_a, relay_c, mid_c, near_c)
    sum_c.start()
    arrived(("b1", 2))
    start_b2(2)
    sum_b.finish(into(next_b))
    sum_d = RingSum(links, "z", next_b, relay_d, mid_d, near_d)
    sum_d.start()
    sum2.across()
    arrived(("b2", 3))
    start_core(3)
    total = through_block(c, 3, total)
    arrived(("b2", 1))
    start_core(1)
    total = through_block(c, 1, total)
    sum_c.forward()
    sum_d.forward()
    arrived(("core", 3))
    total = through_block(1 - c, 3, total)
    arrived(("b2", 2))
    start_core(2)
    total = through_block(c, 2, total)
    arrived(("core", 1))
    total = through_block(1 - c, 1, total)
    sum1.outward()
    sum2.back()

    def result(at):
        def put(half, span, value):
            cols = slice(at, at + value.shape[1])
            rows = slice(half * 16, half * 16 + 16)
            pgrad[rows, cols] = (value * slope[rows, cols]).astype(BF16)

        return put

    sum_c.finish(result(0))
    sum_d.finish(result(next_a.shape[-1]))
    msum.wait_recv()
    mout[...] = (mpart[...] + mr[0]) + (mr[1] + mr[2])
    arrived(("core", 2))
    total = through_block(1 - c, 2, total)
    sum2.outward()
    sum1.last()
    sum2.last()
    sum1.end()
    sum2.end()
    inverse_out[...] = jnp.broadcast_to(inverse, (256, 128))
    drop = inverse * inverse * inverse * (total * (1.0 / 8192))
    drop_out[...] = jnp.broadcast_to(drop, (256, 128))

    for store in stores:
        store.wait()
    for copies in (all_rows, all_back, all_spread, all_low_out, all_low_rows):
        copies.wait_send()
    links.finish()


def big_call(scale_factor, *args):
    dma = pltpu.SemaphoreType.DMA
    wide_a, wide_b = 2560, 2560

    def big(w):
        return [
            pltpu.VMEM((2, 64, w), BF16),
            pltpu.VMEM((2, 64, w), BF16),
            pltpu.VMEM((2, 2, 64, w), BF16),
            pltpu.VMEM((4, 2, 16, w), BF16),
        ]

    def small(w):
        return [
            pltpu.VMEM((2, 16, w), BF16),
            pltpu.VMEM((2, 16, w), BF16),
            pltpu.VMEM((2, 2, 16, w), BF16),
        ]

    def sums():
        return [
            pltpu.VMEM((8, 8192), F32),
            pltpu.VMEM((4, 8, 2048), F32),
            pltpu.VMEM((3, 8, 2048), F32),
            pltpu.VMEM((16, 8, 128), F32),
            pltpu.VMEM((16, 8, 128), F32),
            pltpu.VMEM((4, 16, 8, 128), F32),
            pltpu.VMEM((4, 16, 8, 128), F32),
        ]

    scalar = pl.BlockSpec(memory_space=pltpu.SMEM)
    shape = jax.ShapeDtypeStruct
    return pl.pallas_call(
        functools.partial(big_kernel, scale_factor),
        out_shape=(
            shape((256, 8192), BF16),
            shape((256, 128), BF16),
            shape((256, 128), F32),
            shape((256, 128), F32),
            shape((32, 5120), BF16),
            shape((16, 8192), F32),
            shape((16, 8192), F32),
            shape((16, 256), F32),
        ),
        in_specs=[scalar, scalar] + [VMEM] * 4 + [ANY] * 9,
        out_specs=(ANY,) + (VMEM,) * 7,
        scratch_shapes=[
            pltpu.VMEM((2, 4, 1024, 1024), BF16),
            pltpu.VMEM((8, 256, 1024), BF16),
            pltpu.VMEM((8, 256, 1024), BF16),
            pltpu.VMEM((8, 256, 1024), BF16),
            dma((70,)), dma((70,)), dma((23,)), dma((8,)),
            pltpu.VMEM((256, 1024), BF16),
            pltpu.VMEM((8, 1, 1024), F32),
            pltpu.VMEM((16, 8192), BF16),
            pltpu.VMEM((32, 5120), BF16),
            pltpu.VMEM((16, 5120), BF16),
            pltpu.VMEM((32, 5120), F32),
            pltpu.VMEM((16, 1024), BF16),
            pltpu.VMEM((8, 16, 1024), BF16),
            pltpu.VMEM((8, 16, 1024), BF16),
            pltpu.VMEM((8, 16, 1024), BF16),
            pltpu.VMEM((8, 16, 1024), BF16),
            pltpu.VMEM((8, 16, 1024), BF16),
            pltpu.VMEM((8, 16, 1024), F32),
            pltpu.VMEM((4, 4, 2, 16, 256), BF16),
            pltpu.VMEM((32, 2, 16, 256), BF16),
            pltpu.VMEM((32, 128), BF16),
            pltpu.VMEM((32, 32, 128), BF16),
            pltpu.VMEM((32, 5120), BF16),
            pltpu.VMEM((2, 5120, 256), BF16),
            pltpu.VMEM((16, 256), BF16),
            pltpu.VMEM((16, 32, 128), F32),
            pltpu.VMEM((16, 32, 128), F32),
            pltpu.VMEM((512, 256), BF16),
            pltpu.VMEM((512, 256), BF16),
            pltpu.VMEM((16, 256), F32),
            pltpu.VMEM((3, 16, 256), F32),
            pltpu.VMEM((4, 2, 64, wide_a), BF16),
            pltpu.VMEM((4, 2, 64, wide_b), BF16),
            *big(wide_a), *big(wide_b), *small(wide_a), *small(wide_b),
            pltpu.VMEM((16, 8192), F32),
            pltpu.VMEM((16, 8192), F32),
            *sums(), *sums(),
        ],
        compiler_params=pltpu.CompilerParams(
            collective_id=0, has_side_effects=True, vmem_limit_bytes=67_043_328
        ),
        name="big",
    )(*args)


def finish_kernel(
    mup, hidden, resid, through, sums1, sums2,
    gain_in, down_in, low_in, inverse_in, drop_in, pgrad_in,
    out, pgrad_out, vdown, vup, mdown, mup_out,
    hb, rb, tb, one, two, gain, down_t, low, inverse, drop, pgrad,
    load_sems, out_sems, sum_sems, small_sems,
):
    small = []
    pairs = (
        (gain_in, gain), (down_in, down_t), (low_in, low), (inverse_in, inverse),
        (drop_in, drop), (pgrad_in, pgrad),
    )
    for n, (src, dst) in enumerate(pairs):
        small.append(pltpu.make_async_copy(src, dst, small_sems.at[n]))
        small[n].start()
    loads = []

    def load(k):
        cols = pl.ds(k * 1024, 1024)
        loads.append(
            [
                pltpu.make_async_copy(src.at[:, cols], dst.at[k], load_sems.at[n, k])
                for n, (src, dst) in enumerate(((through, tb), (hidden, hb), (resid, rb)))
            ]
        )
        for copy in loads[k]:
            copy.start()

    for k in range(3):
        load(k)
    sums_in = [
        pltpu.make_async_copy(sums1, one, sum_sems.at[0]),
        pltpu.make_async_copy(sums2, two, sum_sems.at[1]),
    ]
    for copy in small:
        copy.wait()
    mup_out[...] = mup[...]
    stores = []
    for k in range(8):
        cols = slice(k * 1024, (k + 1) * 1024)
        for copy in loads[k]:
            copy.wait()
        if k < 5:
            load(k + 3)
        if k == 4:
            for copy in sums_in:
                copy.start()
        grad = tb[k].astype(F32) + adapter_scale * jnp.dot(
            low[:, 0:16], down_t[:, cols], preferred_element_type=F32
        )
        rows = (
            rb[k].astype(F32)
            + inverse[:, 0:1] * (gain[k] * grad)
            - hb[k].astype(F32) * drop[:, 0:1]
        )
        tb[k] = rows.astype(BF16)
        store = pltpu.make_async_copy(tb.at[k], out.at[:, pl.ds(k * 1024, 1024)], out_sems.at[k])
        store.start()
        stores.append(store)
    for copy in sums_in:
        copy.wait()
    stores += [
        pltpu.make_async_copy(pgrad, pgrad_out, small_sems.at[6]),
        pltpu.make_async_copy(one, vdown, sum_sems.at[2]),
        pltpu.make_async_copy(two.at[:, pl.ds(0, 1024)], vup, sum_sems.at[3]),
        pltpu.make_async_copy(two.at[:, pl.ds(1024, 5120)], mdown, sum_sems.at[4]),
    ]
    for store in stores[8:]:
        store.start()
    for store in stores:
        store.wait()


def finish(*args):
    dma = pltpu.SemaphoreType.DMA
    shape = jax.ShapeDtypeStruct
    return pl.pallas_call(
        finish_kernel,
        out_shape=(
            shape((256, 8192), BF16),
            shape((32, 5120), BF16),
            shape((16, 8192), F32),
            shape((16, 1024), F32),
            shape((16, 5120), F32),
            shape((16, 256), F32),
        ),
        in_specs=[VMEM] + [ANY] * 11,
        out_specs=(ANY, ANY, ANY, ANY, ANY, VMEM),
        scratch_shapes=[
            pltpu.VMEM((8, 256, 1024), BF16),
            pltpu.VMEM((8, 256, 1024), BF16),
            pltpu.VMEM((8, 256, 1024), BF16),
            pltpu.VMEM((16, 8192), F32),
            pltpu.VMEM((16, 8192), F32),
            pltpu.VMEM((8, 1, 1024), F32),
            pltpu.VMEM((16, 8192), BF16),
            pltpu.VMEM((256, 128), BF16),
            pltpu.VMEM((256, 128), F32),
            pltpu.VMEM((256, 128), F32),
            pltpu.VMEM((32, 5120), BF16),
            dma((3, 8)), dma((8,)), dma((5,)), dma((7,)),
        ],
        compiler_params=pltpu.CompilerParams(vmem_limit_bytes=67_043_328),
        name="finish",
    )(*args)


def body(
    hidden,
    residual_gradient,
    value_output_gradient,
    attention_norm_gain,
    value_frozen_weight,
    value_down_factor,
    value_up_factor,
    merger_frozen_weight,
    merger_down_factor,
    merger_up_factor,
    merger_saved_preactivation,
    image_token_counts,
    image_encoder_owner,
    image_first_rows,
):
    scale_factor = 256.0 / (hidden.shape[0] * 128) * adapter_scale
    gain = attention_norm_gain.reshape(8, 1, 1024)
    down_t = value_down_factor.T
    through, low, inverse, drop, pgrad, sums1, sums2, mup_sum = big_call(
        scale_factor,
        image_first_rows,
        image_token_counts,
        image_token_counts.reshape(1, 32),
        image_encoder_owner.reshape(1, 32),
        value_up_factor,
        merger_up_factor,
        value_output_gradient,
        gain,
        down_t,
        merger_saved_preactivation,
        merger_down_factor.T,
        hidden,
        residual_gradient,
        value_frozen_weight,
        merger_frozen_weight,
    )
    layer_input_gradient, preactivation_gradient, vdown, vup, mdown, merger_up_gradient = finish(
        mup_sum,
        hidden,
        residual_gradient,
        through,
        sums1,
        sums2,
        gain,
        down_t,
        low,
        inverse,
        drop,
        pgrad,
    )
    return (
        layer_input_gradient,
        preactivation_gradient,
        vdown.T,
        vup,
        mdown.T,
        merger_up_gradient,
    )


def solution(mesh):
    tokens = P(("dp", "fsdp", "enc"), None)
    features = P(None, ("fsdp", "enc"))
    placed = (
        tokens,
        tokens,
        tokens,
        P(),
        P("fsdp", None),
        P(),
        P(),
        features,
        P(),
        features,
        tokens,
        P("dp"),
        P("dp"),
        P(("dp", "fsdp", "enc")),
    )
    return jax.shard_map(
        body,
        mesh=mesh,
        in_specs=placed,
        out_specs=(tokens, tokens, P(), P(), P(), features),
        check_vma=False,
    )
```

```python
import functools

import jax
import jax.numpy as jnp
from jax import lax
from jax.experimental import pallas as pl
from jax.experimental.pallas import tpu as pltpu
from jax.sharding import PartitionSpec as P

MAXIMG = 16
adapter_scale = 2.0
norm_eps = 1e-06
F32, BF16 = jnp.float32, jnp.bfloat16
MESH = pl.DeviceIdType.MESH
VMEM = pl.BlockSpec(memory_space=pltpu.VMEM)
ANY = pl.BlockSpec(memory_space=pl.ANY)


def dot_nt(a, b):
    return lax.dot_general(a, b, (((1,), (1,)), ((), ())), preferred_element_type=F32)


def dot_tn(a, b):
    return lax.dot_general(a, b, (((0,), (0,)), ((), ())), preferred_element_type=F32)


def wrap(v, n):
    return lax.rem(v + n, n)


def place():
    f = lax.axis_index("fsdp")
    return lax.axis_index("dp"), f // 2, lax.axis_index("enc"), lax.rem(f, 2)


class Links:
    def __init__(self, send_sems, recv_sems):
        self.x, self.y, self.z, self.c = place()
        self.send_sems, self.recv_sems = send_sems, recv_sems
        self.made = []
        self.taken = 0

    def peer(self, axis, step):
        if axis == "x":
            return {"dp": wrap(self.x + step, 4)}
        if axis == "z":
            return {"enc": wrap(self.z + step, 4)}
        if axis == "y":
            return {"fsdp": 2 * wrap(self.y + step, 4) + self.c}
        return {"fsdp": 2 * self.y + 1 - self.c}

    def take(self):
        self.taken += 1
        return self.send_sems.at[self.taken - 1], self.recv_sems.at[self.taken - 1]

    def send(self, axis, step, src, dst):
        return self.group([(axis, step, src, dst)], dst)

    def group(self, sends, whole):
        sems = self.take()
        for axis, step, src, dst in sends:
            self.copy(sems, src, dst, self.peer(axis, step)).start()
        total = self.copy(sems, whole, whole, self.peer(*sends[0][:2]))
        self.made.append(total)
        return total

    def copy(self, sems, src, dst, peer):
        return pltpu.make_async_remote_copy(
            src_ref=src,
            dst_ref=dst,
            send_sem=sems[0],
            recv_sem=sems[1],
            device_id=peer,
            device_id_type=MESH,
        )

    def finish(self):
        for copy in self.made:
            copy.wait_send()

    def meet(self, peers):
        barrier = pltpu.get_barrier_semaphore()
        for axis, step in peers:
            pl.semaphore_signal(barrier, inc=1, device_id=self.peer(axis, step), device_id_type=MESH)
        pl.semaphore_wait(barrier, len(peers))


def chunked(count, act):
    def step(i, carry):
        act(pl.ds(pl.multiple_of(i * 16, 16), 16))
        return carry

    lax.fori_loop(0, count // 16, step, 0)


class RingSum:
    def __init__(self, links, axis, blocks, relay, mid, near):
        self.links, self.axis, self.blocks = links, axis, blocks
        self.relay, self.mid, self.near = relay, mid, near
        m = links.x if axis == "x" else links.y if axis == "y" else links.z
        self.me, self.count = m, blocks.shape[2]

    def start(self):
        send, b, axis = self.links.send, self.blocks, self.axis
        far = wrap(self.me + 2, 4)
        right, left = wrap(self.me + 1, 4), wrap(self.me - 1, 4)
        self.far = [
            send(axis, 1, b.at[far, 0], self.relay.at[0]),
            send(axis, -1, b.at[far, 1], self.relay.at[1]),
        ]
        self.direct = [
            send(axis, 1, b.at[right, 1], self.near.at[0, 1]),
            send(axis, -1, b.at[left, 0], self.near.at[1, 0]),
        ]

    def forward(self):
        for way, step in ((0, 1), (1, -1)):
            self.far[way].wait_recv()
            to = wrap(self.me + step, 4)

            def add(span, way=way, to=to):
                self.mid[way, span] = (
                    self.blocks[to, way, span].astype(F32) + self.relay[way, span].astype(F32)
                ).astype(BF16)

            chunked(self.count, add)
            self.direct.append(
                self.links.send(self.axis, step, self.mid.at[way], self.near.at[way, way])
            )

    def finish(self, put):
        for copy in self.direct:
            copy.wait_recv()
        for half in range(2):

            def add(span, half=half):
                put(
                    half,
                    span,
                    self.blocks[self.me, half, span].astype(F32)
                    + self.near[0, half, span].astype(F32)
                    + self.near[1, half, span].astype(F32),
                )

            chunked(self.count, add)


class AdapterSum:
    def __init__(self, links, src, out, bufs):
        self.links, self.src, self.out = links, src, out
        self.half_in, self.ay, self.ry, self.bxz, self.rxz, self.gy, self.gc = bufs
        self.sems = links.take(), links.take()
        self.m16 = links.x * 4 + links.z
        self.other = pl.ds(pl.multiple_of((1 - links.c) * 8, 8), 8)
        self.mine = pl.ds(pl.multiple_of(links.c * 8, 8), 8)

    def plane(self, k):
        d = lax.rem(self.m16 + k, 16)
        return {"dp": d // 4, "enc": lax.rem(d, 4)}

    def spread(self, k):
        return self.links.copy(
            self.sems[0], self.bxz.at[lax.rem(self.m16 + k, 16)], self.rxz.at[k - 1], self.plane(k)
        )

    def share(self, k):
        here = self.gy.at[self.links.y, self.m16]
        return self.links.copy(self.sems[1], here, here, self.plane(k))

    def total(self, n):
        whole = self.rxz.at[0:15]
        return self.links.copy(self.sems[n], whole, whole, self.plane(1))

    def swap(self):
        self.swapped = self.links.send("c", 0, self.src.at[self.other], self.half_in)

    def along(self):
        self.swapped.wait_recv()
        for b in range(4):
            cols = slice(b * 2048, (b + 1) * 2048)
            self.ay[b] = self.src[self.mine, cols] + self.half_in[:, cols]
        y = self.links.y
        self.sent = self.links.group(
            [("y", k, self.ay.at[wrap(y + k, 4)], self.ry.at[k - 1]) for k in (1, 2, 3)], self.ry
        )

    def across(self):
        self.sent.wait_recv()
        here = self.ay.at[self.links.y]
        for b in range(16):
            cols = slice(b * 128, (b + 1) * 128)
            self.bxz[b] = (here[:, cols] + self.ry[0, :, cols]) + (
                self.ry[1, :, cols] + self.ry[2, :, cols]
            )
        over(1, 16, lambda k: self.spread(k).start())

    def back(self):
        self.total(0).wait_recv()
        value = self.bxz[self.m16]
        for k in range(15):
            value = value + self.rxz[k]
        self.gy[self.links.y, self.m16] = value
        over(1, 16, lambda k: self.share(k).start())

    def outward(self):
        self.total(1).wait_recv()
        here = self.gy.at[self.links.y]
        self.wide = self.links.group(
            [("y", k, here, here) for k in (1, 2, 3)], self.gy.at[0:3]
        )

    def last(self):
        self.wide.wait_recv()
        self.final = self.links.send("c", 0, self.gy, self.gc)
        for b in range(64):
            self.out[self.mine, b * 128 : (b + 1) * 128] = self.gy[b // 16, b % 16]

    def end(self):
        self.final.wait_recv()
        for b in range(64):
            self.out[self.other, b * 128 : (b + 1) * 128] = self.gc[b // 16, b % 16]
        self.total(0).wait_send()
        self.total(1).wait_send()


def over(lo, hi, act):
    def step(j, carry):
        act(j)
        return carry

    lax.fori_loop(lo, hi, step, 0)


def big_kernel(
    scale_factor,
    first_row, counts_s, counts, owners, up, mup,
    v_in, gain_in, down_in, preact_in, md_in, hidden, resid, wsh, wm,
    through_out, low_out_ref, inverse_out, drop_out, pgrad, sums1, sums2, mout,
    wbuf, xb, rb, through, send_sems, recv_sems, local_sems, out_sems,
    v, gain, down_t, preact, md, slope,
    vimg, xsel, rsel, vall, tout, timg, gained, visout, vrecv, actl, alow, act,
    wmb, mup_other, lowp, lowin, rows_own, rows_other, mpart, mr,
    qa, qb,
    relay_a, mid_a, near_a, next_a, relay_b, mid_b, near_b, next_b,
    relay_c, mid_c, near_c, relay_d, mid_d, near_d,
    part1, part2, *rest,
):
    bufs1, bufs2 = rest[:7], rest[7:14]
    links = Links(send_sems, recv_sems)
    x, y, z, c = links.x, links.y, links.z, links.c
    f = 2 * y + c
    me = f * 4 + z

    small = []
    pairs = ((v_in, v), (gain_in, gain), (down_in, down_t), (preact_in, preact), (md_in, md))
    for n, (src, dst) in enumerate(pairs):
        small.append(pltpu.make_async_copy(src, dst, local_sems.at[18 + n]))
        small[n].start()
    own = pltpu.make_async_copy(wsh, wbuf.at[c, 0], local_sems.at[0])
    own.start()
    loads = []
    for k in range(8):
        cols = pl.ds(k * 1024, 1024)
        a = pltpu.make_async_copy(hidden.at[:, cols], xb.at[k], local_sems.at[1 + k])
        b = pltpu.make_async_copy(resid.at[:, cols], rb.at[k], local_sems.at[9 + k])
        a.start()
        b.start()
        loads.append((a, b))
    wm_load = pltpu.make_async_copy(wm, wmb.at[0], local_sems.at[17])
    wm_load.start()

    barrier = pltpu.get_barrier_semaphore()

    def plane_peer(j):
        d = lax.rem(me + j, 32)
        return {"fsdp": d // 4, "enc": lax.rem(d, 4)}

    def greet(j):
        pl.semaphore_signal(barrier, inc=1, device_id=plane_peer(j), device_id_type=MESH)

    def greet_x(j):
        d = 4 + j
        pl.semaphore_signal(
            barrier,
            inc=1,
            device_id={"dp": lax.rem(x + d // 4, 4), "enc": lax.rem(z + d, 4)},
            device_id_type=MESH,
        )

    over(1, 32, greet)
    over(0, 12, greet_x)
    first = first_row[0]
    lane = lax.broadcasted_iota(jnp.int32, (16, 256), 1)
    line = lax.broadcasted_iota(jnp.int32, (16, 256), 0)
    sel = jnp.where(lane == line + first, 1.0, 0.0).astype(BF16)
    small[0].wait()
    vimg[...] = jnp.dot(sel, v[...], preferred_element_type=F32).astype(BF16)
    pl.semaphore_wait(barrier, 43)

    sems_row, sems_back, sems_spread = links.take(), links.take(), links.take()
    sems_low_out, sems_low_row = links.take(), links.take()
    my16 = y * 4 + z

    def row(j):
        return links.copy(sems_row, vimg, vall.at[f], {"fsdp": lax.rem(f + j, 8)})

    def back(j):
        to = lax.rem(f + j, 8)
        return links.copy(sems_back, tout.at[to], timg.at[f], {"fsdp": to})

    def spread(j):
        d = lax.rem(me + j, 32)
        return links.copy(sems_spread, visout.at[d // 8, lax.rem(d, 4)], vrecv.at[me], plane_peer(j))

    def low_out(j):
        return links.copy(sems_low_out, actl, alow.at[me], plane_peer(j))

    def low_row(j):
        d = lax.rem(my16 + j, 16)
        peer = {"fsdp": 2 * (d // 4) + c, "enc": lax.rem(d, 4)}
        return links.copy(sems_low_row, lowp.at[d], lowin.at[my16], peer)

    def all_of(sems, whole):
        return links.copy(sems, whole, whole, plane_peer(1))

    all_rows = all_of(sems_row, vall.at[0:7])
    all_back = all_of(sems_back, timg.at[0:7])
    all_spread = all_of(sems_spread, vrecv.at[0:31])
    all_low_out = all_of(sems_low_out, alow.at[0:31])
    all_low_rows = all_of(sems_low_row, lowin.at[0:15])

    def at(j, start, count):
        return wbuf.at[c, j, pl.ds(pl.multiple_of(start, 16), count)]

    def piece(step):
        return (x * 4 + wrap(z + step, 4)) * 48

    def block(step):
        return wrap(x + step, 4) * 192

    def early(step):
        return 768 + wrap(x + step, 4) * 64

    moved = {}

    def arrived(name):
        moved[name].wait_recv()

    def group(name, rows, sends):
        moved[name] = links.group(sends, wbuf.at[c, 0, 0:rows])

    def start_y1():
        src = at(0, piece(0), 48)
        group("y1", 96, [("y", t, src, at(j, piece(0), 48)) for t, j in ((1, 3), (-1, 1))])

    def start_y2():
        sends = []
        for t, j, start, count in ((1, 3, piece(0), 32), (-1, 1, piece(0) + 32, 16)):
            sends.append(("y", t, at(j, start, count), at(2, start, count)))
        group("y2", 48, sends)

    def start_r1():
        src = at(0, early(0), 64)
        group("r1", 128, [("y", t, src, at(j, early(0), 64)) for t, j in ((1, 3), (-1, 1))])

    def start_r2():
        sends = []
        for t, j, start in ((1, 3, early(0)), (-1, 1, early(0) + 32)):
            sends.append(("y", t, at(j, start, 32), at(2, start, 32)))
        group("r2", 64, sends)

    def start_c1(j):
        group(("c1", j), 128, [same("x", step, j, early(0), 64) for step in (1, -1)])

    def start_c2(j):
        group(
            ("c2", j),
            64,
            [same("x", 1, j, early(-1), 32), same("x", -1, j, early(1) + 32, 32)],
        )

    def same(axis, step, j, start, count):
        here = at(j, start, count)
        return (axis, step, here, here)

    def start_a1(j):
        group(("a1", j), 96, [same("z", step, j, piece(0), 48) for step in (1, -1)])

    def start_a2(j):
        one = 32 if j == 3 else 16
        group(
            ("a2", j),
            48,
            [same("z", 1, j, piece(-1), one), same("z", -1, j, piece(1) + one, 48 - one)],
        )

    def start_b1(j):
        group(("b1", j), 384, [same("x", step, j, block(0), 192) for step in (1, -1)])

    def start_b2(j):
        group(
            ("b2", j),
            192,
            [same("x", 1, j, block(-1), 96), same("x", -1, j, block(1) + 96, 96)],
        )

    def start_core(j):
        if j:
            arrived(("c2", j))
        moved["core", j] = links.send("c", 0, wbuf.at[c, j], wbuf.at[c, j])

    over(1, 8, lambda j: row(j).start())
    own.wait()
    start_y1()
    start_r1()
    wide = links.send("c", 0, wm, wmb.at[1])
    thin = links.send("c", 0, mup, mup_other)
    start_core(0)
    vall[f] = vimg[...]

    for load in small[1:]:
        load.wait()
    low_img = dot_nt(vimg[...], up[...]).astype(BF16)
    squares_img = jnp.zeros((16, 1), F32)
    for k in range(8):
        loads[k][0].wait()
        rows = jnp.dot(sel, xb[k], preferred_element_type=F32)
        xsel[k] = rows.astype(BF16)
        squares_img = squares_img + jnp.sum(rows * rows, axis=1, keepdims=True)
    inverse_img = lax.rsqrt(squares_img * (1.0 / 8192) + norm_eps)

    all_rows.wait_recv()
    tout[...] = dot_nt(vall[...].reshape(128, 1024), wbuf[c, 0]).astype(BF16).reshape(8, 16, 1024)
    over(1, 8, lambda j: back(j).start())
    timg[f] = tout[f]
    arrived("y1")
    start_y2()
    start_a1(3)
    start_a1(1)
    arrived("r1")
    start_r2()
    start_c1(3)
    start_c1(1)

    for k in range(8):
        loads[k][1].wait()
        rsel[k] = jnp.dot(sel, rb[k], preferred_element_type=F32).astype(BF16)
    squares = jnp.zeros((256, 1), F32)
    for k in range(8):
        xs = xb[k].astype(F32)
        squares = squares + jnp.sum(xs * xs, axis=1, keepdims=True)
    inverse = lax.rsqrt(squares * (1.0 / 8192) + norm_eps)

    all_back.wait_recv()
    total_img = jnp.zeros((16, 1), F32)
    for k in range(8):
        grad = timg[k].astype(F32) + adapter_scale * jnp.dot(
            low_img, down_t[:, k * 1024 : (k + 1) * 1024], preferred_element_type=F32
        )
        g = gain[k] * grad
        gained[k] = g
        total_img = total_img + jnp.sum(xsel[k].astype(F32) * g, axis=1, keepdims=True)
    drop_img = inverse_img * inverse_img * inverse_img * (total_img * (1.0 / 8192))
    inside = lax.broadcasted_iota(jnp.int32, (16, 1024), 0) < counts_s[me]
    for k in range(8):
        rows = (
            rsel[k].astype(F32) + inverse_img * gained[k] - xsel[k].astype(F32) * drop_img
        )
        rows = jnp.where(inside, rows, 0.0).astype(BF16)
        for b in range(4):
            visout[k // 2, b, k % 2] = rows[:, b * 256 : (b + 1) * 256]
    over(1, 32, lambda j: spread(j).start())
    vrecv[me] = visout[y, z]

    p = preact[...].astype(F32)
    normal_cdf = 0.5 * (1.0 + lax.erf(p * 0.7071067811865476))
    act[...] = (p * normal_cdf).astype(BF16)
    slope[...] = normal_cdf + p * (jnp.exp(-0.5 * p * p) * 0.3989422804014327)
    actl[...] = jnp.zeros_like(actl)
    actl[:, 0:16] = dot_nt(act[...], md[...]).astype(BF16)
    alow[me] = actl[...]

    arrived("y2")
    start_a1(2)
    arrived("r2")
    start_c1(2)
    arrived(("c1", 3))
    start_c2(3)
    arrived(("c1", 1))
    start_c2(1)
    arrived(("a1", 3))
    start_a2(3)
    arrived(("a1", 1))
    start_a2(1)

    low = dot_nt(v[...], up[...]).astype(BF16)
    low_out_ref[:, 0:16] = low
    low_out_ref[:, 16:128] = jnp.zeros((256, 112), BF16)
    low_t = dot_nt(up[...], v[...]).astype(BF16)
    projected_t = jnp.zeros((16, 256), F32)
    for k in range(8):
        normed = (xb[k].astype(F32) * inverse * gain[k]).astype(BF16)
        part1[:, k * 1024 : (k + 1) * 1024] = scale_factor * jnp.dot(
            low_t, normed, preferred_element_type=F32
        )
        projected_t = projected_t + dot_nt(down_t[:, k * 1024 : (k + 1) * 1024], normed)
    sum1 = AdapterSum(links, part1, sums1, bufs1)
    sum1.swap()
    part2[:, 0:1024] = scale_factor * jnp.dot(
        projected_t.astype(BF16), v[...], preferred_element_type=F32
    )
    part2[:, 6144:8192] = jnp.zeros((16, 2048), F32)

    eye = lax.broadcasted_iota(jnp.int32, (32, 32), 0) == lax.broadcasted_iota(
        jnp.int32, (32, 32), 1
    )
    earlier = lax.broadcasted_iota(jnp.int32, (32, 32), 1) < lax.broadcasted_iota(
        jnp.int32, (32, 32), 0
    )
    counts_f = counts[...].astype(F32)
    owners_f = owners[...].astype(F32)
    owner_col = jnp.sum(jnp.where(eye, owners_f, 0.0), axis=1, keepdims=True)
    count_col = jnp.sum(jnp.where(eye, counts_f, 0.0), axis=1, keepdims=True)
    start_col = jnp.sum(
        jnp.where((owner_col == owners_f) & earlier, counts_f, 0.0), axis=1, keepdims=True
    )
    slot = lax.broadcasted_iota(jnp.int32, (32, 512), 1)
    image = lax.broadcasted_iota(jnp.int32, (32, 512), 0)
    inner = (slot % 16).astype(F32)
    key = (
        jnp.sum(
            jnp.where(
                (slot // 16 == image) & (inner < count_col),
                owner_col * 32.0 + start_col + inner + 1.0,
                0.0,
            ),
            axis=0,
            keepdims=True,
        )
        - 1.0
    )

    all_spread.wait_recv()
    wide.wait_recv()
    thin.wait_recv()
    wm_load.wait()
    r = lax.broadcasted_iota(jnp.int32, (512, 1), 0)
    row_id = ((2 * (r // 128) + c) * 4 + (r // 32) % 4) * 32 + r % 32
    pick = jnp.where(row_id.astype(F32) == key, 1.0, 0.0).astype(BF16)
    rows_own[...] = jnp.dot(
        pick, vrecv[:, c].reshape(512, 256), preferred_element_type=F32
    ).astype(BF16)
    rows_other[...] = jnp.dot(
        pick, vrecv[:, 1 - c].reshape(512, 256), preferred_element_type=F32
    ).astype(BF16)
    low_part = dot_nt(rows_own[...], mup[...]) + dot_nt(rows_other[...], mup_other[...])
    lowp[...] = jnp.zeros_like(lowp)
    lowp[:, :, 0:16] = low_part.reshape(16, 32, 16)
    over(1, 16, lambda j: low_row(j).start())
    over(1, 32, lambda j: low_out(j).start())
    sum1.along()
    arrived(("a2", 3))
    start_b1(3)
    arrived(("a1", 2))
    start_a2(2)
    arrived(("c1", 2))
    start_c2(2)
    low_hi = low_part.astype(BF16)
    low_lo = (low_part - low_hi.astype(F32)).astype(BF16)

    def columns(n):
        cols = pl.ds(pl.multiple_of(n * 512, 512), 512)
        value = dot_nt(rows_own[...], wmb[0, cols]) + dot_nt(rows_other[...], wmb[1, cols])
        value = value + adapter_scale * (
            jnp.dot(low_hi, md[:, cols], preferred_element_type=F32)
            + jnp.dot(low_lo, md[:, cols], preferred_element_type=F32)
        )
        return value.astype(BF16)

    def fill_a(n):
        value = columns(n)
        cols = pl.ds(pl.multiple_of(n * 512, 512), 512)
        for yy in range(4):
            for zz in range(4):
                at_row = yy * 128 + zz * 32
                qa[zz, yy // 2, (yy % 2) * 32 : (yy % 2) * 32 + 32, cols] = value[
                    at_row : at_row + 32
                ]

    def fill_b(n):
        value = columns(n + 5)
        cols = pl.ds(pl.multiple_of(n * 512, 512), 512)
        qb[:, :, :, cols] = value.reshape(4, 2, 64, 512)

    sum_a = RingSum(links, "z", qa, relay_a, mid_a, near_a)
    sum_b = RingSum(links, "y", qb, relay_b, mid_b, near_b)
    over(0, 5, fill_a)
    sum_a.start()
    arrived(("a2", 1))
    start_b1(1)
    over(0, 5, fill_b)
    sum_b.start()
    sum1.across()
    arrived(("a2", 2))
    start_b1(2)

    total = jnp.zeros((256, 1), F32)
    stores = []

    def through_block(cs, j, total):
        k = 2 * lax.rem(y + j, 4) + cs
        value = dot_nt(v[...], wbuf[cs, j]).astype(BF16)
        through[k] = value
        cols = pl.ds(pl.multiple_of(k * 1024, 1024), 1024)
        store = pltpu.make_async_copy(
            through.at[k], through_out.at[:, cols], out_sems.at[len(stores)]
        )
        store.start()
        stores.append(store)
        grad = value.astype(F32) + adapter_scale * jnp.dot(
            low, down_t[:, cols], preferred_element_type=F32
        )
        return total + jnp.sum(xb[k].astype(F32) * (gain[k] * grad), axis=1, keepdims=True)

    all_low_rows.wait_recv()
    lowin[my16] = lowp[my16]
    low_sum = lowin[0]
    for k in range(1, 16):
        low_sum = low_sum + lowin[k]
    low_sum_t = low_sum.T[0:16].astype(BF16)
    part2[:, 1024:6144] = scale_factor * jnp.dot(
        low_sum_t, act[...], preferred_element_type=F32
    )
    sum2 = AdapterSum(links, part2, sums2, bufs2)
    sum2.swap()
    total = through_block(c, 0, total)
    sum2.along()
    arrived(("core", 0))
    total = through_block(1 - c, 0, total)
    sum_a.forward()
    arrived(("b1", 3))
    start_b2(3)

    all_low_out.wait_recv()
    every = lax.broadcasted_iota(jnp.int32, (1024, 1), 0).astype(F32)
    pick_all = jnp.where(every == key, 1.0, 0.0).astype(BF16)
    low_slots = dot_tn(alow[...].reshape(1024, 128), pick_all).astype(BF16)
    mpart[...] = scale_factor * jnp.dot(
        low_slots[0:16], vrecv[:, c].reshape(512, 256), preferred_element_type=F32
    )
    msum = links.group([("x", k, mpart, mr.at[k - 1]) for k in (1, 2, 3)], mr)
    sum_b.forward()
    arrived(("b1", 1))
    start_b2(1)
    def into(ref):
        def put(half, span, value):
            i = span.start // 16
            ref[2 * half + i // 2, lax.rem(i, 2)] = value.astype(BF16)

        return put

    sum1.back()
    sum_a.finish(into(next_a))
    sum_c = RingSum(links, "y", next_a, relay_c, mid_c, near_c)
    sum_c.start()
    arrived(("b1", 2))
    start_b2(2)
    sum_b.finish(into(next_b))
    sum_d = RingSum(links, "z", next_b, relay_d, mid_d, near_d)
    sum_d.start()
    sum2.across()
    arrived(("b2", 3))
    start_core(3)
    total = through_block(c, 3, total)
    arrived(("b2", 1))
    start_core(1)
    sum2.back()
    total = through_block(c, 1, total)
    sum_c.forward()
    sum_d.forward()
    arrived(("core", 3))
    total = through_block(1 - c, 3, total)
    arrived(("b2", 2))
    start_core(2)
    total = through_block(c, 2, total)
    sum2.outward()
    sum1.outward()
    arrived(("core", 1))
    total = through_block(1 - c, 1, total)

    def result(at):
        def put(half, span, value):
            cols = slice(at, at + value.shape[1])
            rows = slice(half * 16, half * 16 + 16)
            pgrad[rows, cols] = (value * slope[rows, cols]).astype(BF16)

        return put

    sum_c.finish(result(0))
    sum_d.finish(result(next_a.shape[-1]))
    msum.wait_recv()
    mout[...] = (mpart[...] + mr[0]) + (mr[1] + mr[2])
    arrived(("core", 2))
    total = through_block(1 - c, 2, total)
    sum1.last()
    sum2.last()
    sum1.end()
    sum2.end()
    inverse_out[...] = jnp.broadcast_to(inverse, (256, 128))
    drop = inverse * inverse * inverse * (total * (1.0 / 8192))
    drop_out[...] = jnp.broadcast_to(drop, (256, 128))

    for store in stores:
        store.wait()
    for copies in (all_rows, all_back, all_spread, all_low_out, all_low_rows):
        copies.wait_send()
    links.finish()


def big_call(scale_factor, *args):
    dma = pltpu.SemaphoreType.DMA
    wide_a, wide_b = 2560, 2560

    def big(w):
        return [
            pltpu.VMEM((2, 64, w), BF16),
            pltpu.VMEM((2, 64, w), BF16),
            pltpu.VMEM((2, 2, 64, w), BF16),
            pltpu.VMEM((4, 2, 16, w), BF16),
        ]

    def small(w):
        return [
            pltpu.VMEM((2, 16, w), BF16),
            pltpu.VMEM((2, 16, w), BF16),
            pltpu.VMEM((2, 2, 16, w), BF16),
        ]

    def sums():
        return [
            pltpu.VMEM((8, 8192), F32),
            pltpu.VMEM((4, 8, 2048), F32),
            pltpu.VMEM((3, 8, 2048), F32),
            pltpu.VMEM((16, 8, 128), F32),
            pltpu.VMEM((16, 8, 128), F32),
            pltpu.VMEM((4, 16, 8, 128), F32),
            pltpu.VMEM((4, 16, 8, 128), F32),
        ]

    scalar = pl.BlockSpec(memory_space=pltpu.SMEM)
    shape = jax.ShapeDtypeStruct
    return pl.pallas_call(
        functools.partial(big_kernel, scale_factor),
        out_shape=(
            shape((256, 8192), BF16),
            shape((256, 128), BF16),
            shape((256, 128), F32),
            shape((256, 128), F32),
            shape((32, 5120), BF16),
            shape((16, 8192), F32),
            shape((16, 8192), F32),
            shape((16, 256), F32),
        ),
        in_specs=[scalar, scalar] + [VMEM] * 4 + [ANY] * 9,
        out_specs=(ANY,) + (VMEM,) * 7,
        scratch_shapes=[
            pltpu.VMEM((2, 4, 1024, 1024), BF16),
            pltpu.VMEM((8, 256, 1024), BF16),
            pltpu.VMEM((8, 256, 1024), BF16),
            pltpu.VMEM((8, 256, 1024), BF16),
            dma((70,)), dma((70,)), dma((23,)), dma((8,)),
            pltpu.VMEM((256, 1024), BF16),
            pltpu.VMEM((8, 1, 1024), F32),
            pltpu.VMEM((16, 8192), BF16),
            pltpu.VMEM((32, 5120), BF16),
            pltpu.VMEM((16, 5120), BF16),
            pltpu.VMEM((32, 5120), F32),
            pltpu.VMEM((16, 1024), BF16),
            pltpu.VMEM((8, 16, 1024), BF16),
            pltpu.VMEM((8, 16, 1024), BF16),
            pltpu.VMEM((8, 16, 1024), BF16),
            pltpu.VMEM((8, 16, 1024), BF16),
            pltpu.VMEM((8, 16, 1024), BF16),
            pltpu.VMEM((8, 16, 1024), F32),
            pltpu.VMEM((4, 4, 2, 16, 256), BF16),
            pltpu.VMEM((32, 2, 16, 256), BF16),
            pltpu.VMEM((32, 128), BF16),
            pltpu.VMEM((32, 32, 128), BF16),
            pltpu.VMEM((32, 5120), BF16),
            pltpu.VMEM((2, 5120, 256), BF16),
            pltpu.VMEM((16, 256), BF16),
            pltpu.VMEM((16, 32, 128), F32),
            pltpu.VMEM((16, 32, 128), F32),
            pltpu.VMEM((512, 256), BF16),
            pltpu.VMEM((512, 256), BF16),
            pltpu.VMEM((16, 256), F32),
            pltpu.VMEM((3, 16, 256), F32),
            pltpu.VMEM((4, 2, 64, wide_a), BF16),
            pltpu.VMEM((4, 2, 64, wide_b), BF16),
            *big(wide_a), *big(wide_b), *small(wide_a), *small(wide_b),
            pltpu.VMEM((16, 8192), F32),
            pltpu.VMEM((16, 8192), F32),
            *sums(), *sums(),
        ],
        compiler_params=pltpu.CompilerParams(
            collective_id=0, has_side_effects=True, vmem_limit_bytes=67_043_328
        ),
        name="big",
    )(*args)


def finish_kernel(
    mup, hidden, resid, through, sums1, sums2,
    gain_in, down_in, low_in, inverse_in, drop_in, pgrad_in,
    out, pgrad_out, vdown, vup, mdown, mup_out,
    hb, rb, tb, one, two, gain, down_t, low, inverse, drop, pgrad,
    load_sems, out_sems, sum_sems, small_sems,
):
    small = []
    pairs = (
        (gain_in, gain), (down_in, down_t), (low_in, low), (inverse_in, inverse),
        (drop_in, drop), (pgrad_in, pgrad),
    )
    for n, (src, dst) in enumerate(pairs):
        small.append(pltpu.make_async_copy(src, dst, small_sems.at[n]))
        small[n].start()
    loads = []

    def load(k):
        cols = pl.ds(k * 1024, 1024)
        loads.append(
            [
                pltpu.make_async_copy(src.at[:, cols], dst.at[k], load_sems.at[n, k])
                for n, (src, dst) in enumerate(((through, tb), (hidden, hb), (resid, rb)))
            ]
        )
        for copy in loads[k]:
            copy.start()

    for k in range(3):
        load(k)
    sums_in = [
        pltpu.make_async_copy(sums1, one, sum_sems.at[0]),
        pltpu.make_async_copy(sums2, two, sum_sems.at[1]),
    ]
    for copy in small:
        copy.wait()
    mup_out[...] = mup[...]
    stores = []
    for k in range(8):
        cols = slice(k * 1024, (k + 1) * 1024)
        for copy in loads[k]:
            copy.wait()
        if k < 5:
            load(k + 3)
        if k == 4:
            for copy in sums_in:
                copy.start()
        grad = tb[k].astype(F32) + adapter_scale * jnp.dot(
            low[:, 0:16], down_t[:, cols], preferred_element_type=F32
        )
        rows = (
            rb[k].astype(F32)
            + inverse[:, 0:1] * (gain[k] * grad)
            - hb[k].astype(F32) * drop[:, 0:1]
        )
        tb[k] = rows.astype(BF16)
        store = pltpu.make_async_copy(tb.at[k], out.at[:, pl.ds(k * 1024, 1024)], out_sems.at[k])
        store.start()
        stores.append(store)
    for copy in sums_in:
        copy.wait()
    stores += [
        pltpu.make_async_copy(pgrad, pgrad_out, small_sems.at[6]),
        pltpu.make_async_copy(one, vdown, sum_sems.at[2]),
        pltpu.make_async_copy(two.at[:, pl.ds(0, 1024)], vup, sum_sems.at[3]),
        pltpu.make_async_copy(two.at[:, pl.ds(1024, 5120)], mdown, sum_sems.at[4]),
    ]
    for store in stores[8:]:
        store.start()
    for store in stores:
        store.wait()


def finish(*args):
    dma = pltpu.SemaphoreType.DMA
    shape = jax.ShapeDtypeStruct
    return pl.pallas_call(
        finish_kernel,
        out_shape=(
            shape((256, 8192), BF16),
            shape((32, 5120), BF16),
            shape((16, 8192), F32),
            shape((16, 1024), F32),
            shape((16, 5120), F32),
            shape((16, 256), F32),
        ),
        in_specs=[VMEM] + [ANY] * 11,
        out_specs=(ANY, ANY, ANY, ANY, ANY, VMEM),
        scratch_shapes=[
            pltpu.VMEM((8, 256, 1024), BF16),
            pltpu.VMEM((8, 256, 1024), BF16),
            pltpu.VMEM((8, 256, 1024), BF16),
            pltpu.VMEM((16, 8192), F32),
            pltpu.VMEM((16, 8192), F32),
            pltpu.VMEM((8, 1, 1024), F32),
            pltpu.VMEM((16, 8192), BF16),
            pltpu.VMEM((256, 128), BF16),
            pltpu.VMEM((256, 128), F32),
            pltpu.VMEM((256, 128), F32),
            pltpu.VMEM((32, 5120), BF16),
            dma((3, 8)), dma((8,)), dma((5,)), dma((7,)),
        ],
        compiler_params=pltpu.CompilerParams(vmem_limit_bytes=67_043_328),
        name="finish",
    )(*args)


def body(
    hidden,
    residual_gradient,
    value_output_gradient,
    attention_norm_gain,
    value_frozen_weight,
    value_down_factor,
    value_up_factor,
    merger_frozen_weight,
    merger_down_factor,
    merger_up_factor,
    merger_saved_preactivation,
    image_token_counts,
    image_encoder_owner,
    image_first_rows,
):
    scale_factor = 256.0 / (hidden.shape[0] * 128) * adapter_scale
    gain = attention_norm_gain.reshape(8, 1, 1024)
    down_t = value_down_factor.T
    through, low, inverse, drop, pgrad, sums1, sums2, mup_sum = big_call(
        scale_factor,
        image_first_rows,
        image_token_counts,
        image_token_counts.reshape(1, 32),
        image_encoder_owner.reshape(1, 32),
        value_up_factor,
        merger_up_factor,
        value_output_gradient,
        gain,
        down_t,
        merger_saved_preactivation,
        merger_down_factor.T,
        hidden,
        residual_gradient,
        value_frozen_weight,
        merger_frozen_weight,
    )
    layer_input_gradient, preactivation_gradient, vdown, vup, mdown, merger_up_gradient = finish(
        mup_sum,
        hidden,
        residual_gradient,
        through,
        sums1,
        sums2,
        gain,
        down_t,
        low,
        inverse,
        drop,
        pgrad,
    )
    return (
        layer_input_gradient,
        preactivation_gradient,
        vdown.T,
        vup,
        mdown.T,
        merger_up_gradient,
    )


def solution(mesh):
    tokens = P(("dp", "fsdp", "enc"), None)
    features = P(None, ("fsdp", "enc"))
    placed = (
        tokens,
        tokens,
        tokens,
        P(),
        P("fsdp", None),
        P(),
        P(),
        features,
        P(),
        features,
        tokens,
        P("dp"),
        P("dp"),
        P(("dp", "fsdp", "enc")),
    )
    return jax.shard_map(
        body,
        mesh=mesh,
        in_specs=placed,
        out_specs=(tokens, tokens, P(), P(), P(), features),
        check_vma=False,
    )
```
